128 devices in a mesh: src: 4 (over y), tgt: 32 (over x, z, core).
Axes of the slice: x: 4, y: 4, z: 4, core: 2. Of those that a mesh axis runs over, the one named last changes fastest.
Arguments:
- source_pca: float32 [64, 16384], P(None, 'src'), may hold values from -6 to 6
- target_pca: float32 [64, 32768], P(None, 'tgt'), may hold values from -6 to 6
- source_labels: int32 [16384], P('src'), may hold values from 0 to 63, as said below
- target_labels: int32 [32768], P('tgt'), may hold values from 0 to 63, as said below
- block_mask: int32 [64, 64], replicated, may hold values from 0 to 1, as said below
Outputs:
- source_projection: float32 [64, 16384], P(None, ('src', 'tgt'))
- target_projection: float32 [64, 32768], P(None, 'tgt')
The draws below stay inside these ranges and needn't reach their ends.
Inputs may be any that keep to these rules, and one draw needn't show every extreme that they name: `source_labels`: each aligned block of 4096 consecutive source cells holds every one of the 64 clusters. `target_labels`: each aligned block of 1024 consecutive target cells holds every one of the 64 clusters. `block_mask`: entries are 0 or 1, and the diagonal is all ones.
All inputs are finite; a program needn't handle non-finite values.
Results may differ from the reference program's by a relative error of at most 0.0003.
Values sent between devices are 32-bit elements; how exact they have to be, the bound alone decides.
A program may use at most 64 MiB of HBM per device.

```python
import math
import jax
import jax.numpy as jnp
from jax import lax

D = 64
K = 64
ITERS = 2
RS = 4096
CT = 1024
NS = 16384
NT = 32768


def covered_labels(key, total, block):
    shards = total // block
    keys = jax.random.split(key, 3)
    labels = jax.random.randint(keys[0], (shards, block), 0, K)
    cover = jax.vmap(lambda k: jax.random.permutation(k, K))(jax.random.split(keys[1], shards))
    labels = labels.at[:, :K].set(cover)
    labels = jax.vmap(lambda k, row: jax.random.permutation(k, row))(jax.random.split(keys[2], shards), labels)
    return labels.reshape(total).astype(jnp.int32)


def draw_source_labels(key, part):
    return covered_labels(jax.random.fold_in(key, 11), NS, RS)


def draw_target_labels(key, part):
    return covered_labels(jax.random.fold_in(key, 23), NT, CT)


def draw_block_mask(key, part):
    picks = jax.random.randint(jax.random.fold_in(key, 37), (K, K), 0, 4) == 0
    diagonal = jnp.arange(K)[:, None] == jnp.arange(K)[None, :]
    return jnp.where(picks | diagonal, 1, 0).astype(jnp.int32)


def draw_source_pca(key, part):
    keys = jax.random.split(jax.random.fold_in(key, 53), 1)
    values = jnp.clip(jax.random.normal(keys[0], (D, NS), jnp.float32), -6.0, 6.0)
    return values.astype(jnp.float32)


def block_levels(stream_key, dims, pieces, least, high):
    def one(axis_at, blocks):
        steps = jax.random.uniform(jax.random.fold_in(jax.random.fold_in(stream_key, 6), axis_at), (blocks,), jnp.float32, least / len(pieces), high / len(pieces))
        return jnp.repeat(jnp.exp(steps), dims[axis_at] // blocks).reshape((-1,) + (1,) * (len(dims) - axis_at - 1))

    loudness = one(*pieces[0])
    for cut in pieces[1:]:
        loudness = loudness * one(*cut)
    return loudness


def noise(key, shape, scale, reach, cuts=(), dtype=jnp.bfloat16):
    level = block_levels(key, shape, cuts, -0.22, 0.18) if cuts else 1.0
    result = jax.random.normal(key, shape, jnp.float32) * scale * level
    return jnp.minimum(jnp.maximum(result, -reach), reach).astype(dtype)


def setup_inputs(seed: int = 0) -> dict:
    key_of = jax.random.split(jax.random.key(seed), 6)
    source_pca = draw_source_pca(jax.random.fold_in(key_of[5], 71), 0)
    target_pca = noise(key_of[1], (D, NT), 1.0, 6.0, ((1, 32),), jnp.float32)
    source_labels = draw_source_labels(jax.random.fold_in(key_of[5], 71), 0)
    target_labels = draw_target_labels(jax.random.fold_in(key_of[5], 71), 0)
    block_mask = draw_block_mask(jax.random.fold_in(key_of[5], 71), 0)
    return {"source_pca": source_pca, "target_pca": target_pca, "source_labels": source_labels, "target_labels": target_labels, "block_mask": block_mask}


EPSILON = 0.05
FLOOR = -1.0e30


def costs(xb, yt):
    cross = lax.dot_general(xb, yt, (((0,), (0,)), ((), ())), precision=lax.Precision.HIGHEST)
    return (jnp.sum(xb * xb, 0)[:, None] + jnp.sum(yt * yt, 0)[None, :] - 2.0 * cross) / D


def reference(source_pca, target_pca, source_labels, target_labels, block_mask):
    rblock = min(512, RS)
    nblock = NS // rblock
    xblocks = source_pca.reshape(D, nblock, rblock).transpose(1, 0, 2)
    lblocks = source_labels.reshape(nblock, rblock)

    def logits(xb, lab, shift_rows, shift_cols):
        allowed = block_mask[lab][:, target_labels] > 0
        value = (shift_rows[:, None] + shift_cols[None, :] - costs(xb, target_pca)) / EPSILON
        return jnp.where(allowed, value, -jnp.inf)

    zero_rows = jnp.zeros((rblock,), jnp.float32)
    zero_cols = jnp.zeros((NT,), jnp.float32)
    g_pot = jnp.zeros((NT,), jnp.float32)
    f_pot = jnp.zeros((NS,), jnp.float32)
    for step in range(ITERS):
        def row_pass(item):
            xb, lab = item
            z = logits(xb, lab, zero_rows, g_pot)
            peak = jnp.max(z, 1)
            return peak + jnp.log(jnp.sum(jnp.exp(z - peak[:, None]), 1))

        lse = lax.map(row_pass, (xblocks, lblocks)).reshape(NS)
        f_pot = -EPSILON * math.log(NS) - EPSILON * lse
        fblocks = f_pot.reshape(nblock, rblock)

        def col_step(carry, item):
            peak, total = carry
            xb, lab, fb = item
            z = logits(xb, lab, fb, zero_cols)
            newer = jnp.maximum(peak, jnp.max(z, 0))
            total = total * jnp.exp(peak - newer) + jnp.sum(jnp.exp(z - newer[None, :]), 0)
            return (newer, total), None

        init = (jnp.full((NT,), FLOOR, jnp.float32), jnp.zeros((NT,), jnp.float32))
        (peak, total), unused = lax.scan(col_step, init, (xblocks, lblocks, fblocks))
        g_pot = -EPSILON * math.log(NT) - EPSILON * (peak + jnp.log(total))

    fblocks = f_pot.reshape(nblock, rblock)

    def proj_step(carry, item):
        peak, total, weighted = carry
        xb, lab, fb = item
        z = logits(xb, lab, fb, g_pot)
        rpeak = jnp.max(z, 1)
        rprob = jnp.exp(z - rpeak[:, None])
        rows = lax.dot_general(target_pca, rprob, (((1,), (1,)), ((), ())), precision=lax.Precision.HIGHEST)
        rows = rows / jnp.sum(rprob, 1)[None, :]
        newer = jnp.maximum(peak, jnp.max(z, 0))
        cprob = jnp.exp(z - newer[None, :])
        scale = jnp.exp(peak - newer)
        total = total * scale + jnp.sum(cprob, 0)
        weighted = weighted * scale[None, :] + jnp.dot(xb, cprob, precision=lax.Precision.HIGHEST)
        return (newer, total, weighted), rows

    init = (jnp.full((NT,), FLOOR, jnp.float32), jnp.zeros((NT,), jnp.float32), jnp.zeros((D, NT), jnp.float32))
    (peak, total, weighted), rows = lax.scan(proj_step, init, (xblocks, lblocks, fblocks))
    source_projection = rows.transpose(1, 0, 2).reshape(D, NS)
    target_projection = weighted / total[None, :]
    return source_projection, target_projection
```

```python
import functools
import math

import jax
import jax.numpy as jnp
from jax import lax
from jax.experimental import pallas as pl
from jax.experimental.pallas import tpu as pltpu
from jax.sharding import PartitionSpec as P

ITERS = 2
EPSILON = 0.05
BARRED = -(2.0**100)
MESH = pl.DeviceIdType.MESH
F32 = jnp.float32
BF16 = jnp.bfloat16
LANES = 128
GROUP = 8
PAD = 72


def in_three(value):
    first = value.astype(BF16)
    rest = value - first.astype(F32)
    second = rest.astype(BF16)
    third = (rest - second.astype(F32)).astype(BF16)
    return first, second, third


def in_two(value):
    first = value.astype(BF16)
    return first, (value - first.astype(F32)).astype(BF16)


def turned(row):
    return jnp.broadcast_to(row, (LANES, LANES)).T


def lse_of(parts):
    top = functools.reduce(jnp.maximum, parts)
    return top + jnp.log2(sum(jnp.exp2(p - top) for p in parts))


def span(index, size):
    return pl.ds(pl.multiple_of(index * size, size), size)


def kernel(S, T, x_ref, y_ref, sl_ref, tl_ref, mask_ref, so_ref, to_ref,
           xa, ya, zr, ehi, elo, frow, mp, mb, sp, sb, xw, yw,
           lbuf, lrec, lpair, lprec, mbuf, gbuf, grec,
           rbuf, rrec, rpair, rprec, cbuf, crec,
           wbuf, wrec, tbuf, trec, sbuf, prec, pbuf, srec,
           lsend, lrecv, psend, precv, gsend, grecv,
           rsend, rrecv, qsend, qrecv, csend, crecv,
           wsend, wrecv, tsend, trecv, bsend, brecv, ssend, srecv):
    dims, R = x_ref.shape
    C = y_ref.shape[1]
    G = T // 2
    QW = C // S
    CB = C // LANES
    RB = R // LANES
    scale = math.log2(math.e) / (EPSILON * dims)
    me_s, me_t = lax.axis_index("src"), lax.axis_index("tgt")
    core = lax.rem(me_t, 2)
    chip = me_t // 2
    partner = me_t + 1 - 2 * core

    def mate(o):
        return (me_s, lax.rem(me_t + 2 * o, T))

    def above(o):
        return (lax.rem(me_s + o, S), me_t)

    pair = (me_s, partner)
    everyone = [mate(o) for o in range(1, G)] + [above(o) for o in range(1, S)] + [pair]
    barrier = pltpu.get_barrier_semaphore()
    for device in everyone:
        pl.semaphore_signal(barrier, inc=1, device_id=device, device_id_type=MESH)

    def remote(src, dst, send, recv, device):
        return pltpu.make_async_remote_copy(
            src_ref=src, dst_ref=dst, send_sem=send, recv_sem=recv,
            device_id=device, device_id_type=MESH)

    def to_mates(src, dst, send, recv):
        return [remote(src, dst.at[o - 1], send.at[o - 1], recv.at[o - 1], mate(o))
                for o in range(1, G)]

    def to_column(src, dst, send, recv):
        return [remote(src, dst.at[o - 1], send.at[o - 1], recv.at[o - 1], above(o))
                for o in range(1, S)]

    def begin(copies):
        for copy in copies:
            copy.start()

    def finish(copies):
        for copy in copies:
            copy.wait()

    XC = 512

    def prepare_source(c, _):
        at = span(c, XC)
        x = x_ref[:, at]
        x1, x2, x3 = in_three(x)
        for k, part in enumerate((x1, x2, x1, x2, x3, x1)):
            xa[k * dims:(k + 1) * dims, at] = part
        ids = lax.broadcasted_iota(jnp.int32, (dims, XC), 0)
        xa[6 * dims:7 * dims, at] = jnp.where(ids == sl_ref[:, at], 1.0, 0.0).astype(BF16)
        n1, n2, n3 = (p.astype(F32) for p in in_three(-scale * jnp.sum(x * x, 0, keepdims=True)))
        norm = jnp.where(ids == 3, n1, jnp.where(ids == 4, n2, jnp.where(ids == 5, n3, 0.0)))
        xa[7 * dims:8 * dims, at] = jnp.where(ids < 3, 1.0, norm).astype(BF16)
        return 0

    lax.fori_loop(0, R // XC, prepare_source, 0)

    y = y_ref[...]
    y1, y2, y3 = (p.astype(F32) for p in in_three(2.0 * scale * y))
    ids = lax.broadcasted_iota(jnp.int32, (dims, C), 0)
    onehot = jnp.where(ids == tl_ref[...], 1.0, 0.0).astype(BF16)
    allowed = jnp.dot(mask_ref[...].astype(F32).astype(BF16), onehot, preferred_element_type=F32)
    penalty = jnp.where(allowed > 0.5, 0.0, BARRED)
    n1, n2, n3 = (p.astype(F32) for p in in_three(-scale * jnp.sum(y * y, 0, keepdims=True)))
    norm = jnp.where(ids == 0, n1, jnp.where(ids == 1, n2, jnp.where(ids == 2, n3, 0.0)))
    norm = jnp.where((ids >= 3) & (ids < 6), 1.0, norm)
    for k, (a, b) in enumerate(((y1, y1), (y2, y2), (y1, y3), (penalty, norm))):
        ya[:, k * LANES:(k + 1) * LANES] = jnp.concatenate([a, b], 0).T.astype(BF16)

    def first_rows(i, _):
        at = span(i, 2 * LANES)
        z = jnp.dot(ya[...], xa[:, at], preferred_element_type=F32)
        zr[:, at] = z
        top = jnp.max(z, 0, keepdims=True)
        lse = top + jnp.log2(jnp.sum(jnp.exp2(z - top), 0, keepdims=True))
        lbuf[pl.ds(2 * i, 1), :] = lse[:, :LANES]
        lbuf[pl.ds(2 * i + 1, 1), :] = lse[:, LANES:]
        return 0

    lax.fori_loop(0, R // (2 * LANES), first_rows, 0)

    pl.semaphore_wait(barrier, len(everyone))
    copies = to_mates(lbuf, lrec, lsend, lrecv)
    begin(copies)
    finish(copies)
    lpair[...] = lse_of([lbuf[...]] + [lrec[o] for o in range(G - 1)])
    copy = remote(lpair, lprec, psend, precv, pair)
    copy.start()
    copy.wait()
    f = -math.log2(R * S) - lse_of([lpair[...], lprec[...]])
    for q in range(RB):
        frow[:, q * LANES:(q + 1) * LANES] = jnp.broadcast_to(f[q:q + 1, :], (GROUP, LANES))

    def chunks(q):
        return slice(q * LANES, (q + 1) * LANES)

    def peaks(j, _):
        at = span(j, GROUP)
        mp[at, :] = functools.reduce(
            jnp.maximum, [zr[at, chunks(q)] + frow[:, chunks(q)] for q in range(RB)])
        return 0

    lax.fori_loop(0, C // GROUP, peaks, 0)
    for b in range(CB):
        rows = slice(b * LANES, (b + 1) * LANES)
        top = jnp.max(mp[rows, :].T, 0, keepdims=True)
        mbuf[b:b + 1, :] = top
        mb[rows, :] = turned(top)

    def weigh(j, _):
        at = span(j, GROUP)
        peak = mb[at, :]
        total = None
        for q in range(RB):
            e = jnp.exp2(zr[at, chunks(q)] + frow[:, chunks(q)] - peak)
            zr[at, chunks(q)] = e
            total = e if total is None else total + e
        sp[at, :] = total
        return 0

    lax.fori_loop(0, C // GROUP, weigh, 0)
    for b in range(CB):
        rows = slice(b * LANES, (b + 1) * LANES)
        total = jnp.sum(sp[rows, :].T, 0, keepdims=True)
        gbuf[b:b + 1, :] = mbuf[b:b + 1, :] + jnp.log2(total)

    copies = to_column(gbuf, grec, gsend, grecv)
    begin(copies)

    def halve(j, _):
        at = span(j, 2 * GROUP)
        ehi[at, :], elo[at, :] = in_two(zr[at, :])
        return 0

    lax.fori_loop(0, C // (2 * GROUP), halve, 0)
    finish(copies)
    lse = lse_of([gbuf[...]] + [grec[o] for o in range(S - 1)])
    sig = jnp.exp2(mbuf[...] - lse)
    mbuf[...] = sig
    for b in range(CB):
        sb[b * LANES:(b + 1) * LANES, :] = turned(sig[b:b + 1, :])

    RC = min(2048, R)
    for h in range(R // RC):

        def mass(j, acc):
            at = span(j, GROUP)
            weight = sb[at, :]
            return tuple(
                acc[q] + zr[at, h * RC + q * LANES:h * RC + (q + 1) * LANES] * weight
                for q in range(RC // LANES))

        acc = lax.fori_loop(
            0, C // GROUP, mass,
            tuple(jnp.zeros((GROUP, LANES), F32) for q in range(RC // LANES)))
        for q, part in enumerate(acc):
            at = h * (RC // LANES) + q
            rbuf[at:at + 1, :] = jnp.sum(part, 0, keepdims=True)

    copies = to_mates(rbuf, rrec, rsend, rrecv)
    begin(copies)
    finish(copies)
    rpair[...] = rbuf[...] + sum(rrec[o] for o in range(G - 1))
    copy = remote(rpair, rprec, qsend, qrecv, pair)
    copy.start()
    copy.wait()
    a = (C * T / (R * S)) / (rpair[...] + rprec[...])
    for q in range(RB):
        frow[:, chunks(q)] = jnp.broadcast_to(a[q:q + 1, :], (GROUP, LANES))

    def sums(j, _):
        at = span(j, GROUP)
        total = None
        for q in range(RB):
            e = zr[at, chunks(q)] * frow[:, chunks(q)]
            total = e if total is None else total + e
        sp[at, :] = total
        return 0

    lax.fori_loop(0, C // GROUP, sums, 0)
    for b in range(CB):
        rows = slice(b * LANES, (b + 1) * LANES)
        cbuf[b:b + 1, :] = sig[b:b + 1, :] * jnp.sum(sp[rows, :].T, 0, keepdims=True)
    copies = to_column(cbuf, crec, csend, crecv)
    begin(copies)

    tail = lax.broadcasted_iota(jnp.int32, (2 * GROUP, LANES), 0)

    def with_mass(dst, at, value, mass):
        hi, lo = in_two(value)
        dst[0:dims, at] = hi
        dst[dims:2 * dims, at] = lo
        m1, m2 = (p.astype(F32) for p in in_two(mass))
        dst[2 * dims:2 * dims + 2 * GROUP, at] = jnp.where(
            tail == 0, m1, jnp.where(tail == 1, m2, 0.0)).astype(BF16)

    for q in range(RB):
        with_mass(xw, chunks(q), x_ref[:, chunks(q)] * a[q:q + 1, :], a[q:q + 1, :])

    def folded(out):
        value = out[0:dims] + out[dims:2 * dims]
        mass = jnp.sum(out[2 * dims:], 0, keepdims=True)
        return value, mass

    across = (((1,), (1,)), ((), ()))

    def target_sums(k, _):
        at = span(k, QW)
        value, mass = folded(
            lax.dot_general(xw[...], ehi[at, :], across, preferred_element_type=F32)
            + lax.dot_general(xw[...], elo[at, :], across, preferred_element_type=F32))
        for b in range(QW // LANES):
            row = mbuf[pl.ds(k * (QW // LANES) + b, 1), :]
            wbuf[k, 0:dims, chunks(b)] = value[:, chunks(b)] * row
            wbuf[k, dims:PAD, chunks(b)] = jnp.broadcast_to(
                mass[:, chunks(b)] * row, (PAD - dims, LANES))
        return 0

    lax.fori_loop(0, S, target_sums, 0)
    wcopies = [
        remote(wbuf.at[lax.rem(me_s + o, S)], wrec.at[o - 1], wsend.at[o - 1], wrecv.at[o - 1],
               above(o)) for o in range(1, S)]
    begin(wcopies)
    finish(copies)
    factor = sig / (cbuf[...] + sum(crec[o] for o in range(S - 1)))
    for b in range(CB):
        row = factor[b:b + 1, :]
        with_mass(yw, chunks(b), y_ref[:, chunks(b)] * row, row)

    def to_partner(o):
        return remote(sbuf.at[o, 1 - core], prec.at[o], bsend.at[o], brecv.at[o], pair)

    def to_owner(o):
        return remote(pbuf.at[o], srec.at[o - 1], ssend.at[o - 1], srecv.at[o - 1], mate(o))

    def source_sums(o):
        at = span(lax.rem(chip + o, G), 2 * LANES)
        value, mass = folded(
            jnp.dot(yw[...], ehi[:, at], preferred_element_type=F32)
            + jnp.dot(yw[...], elo[:, at], preferred_element_type=F32))
        for k in range(2):
            sbuf[o, k, 0:dims, :] = value[:, chunks(k)]
            sbuf[o, k, dims:PAD, :] = jnp.broadcast_to(mass[:, chunks(k)], (PAD - dims, LANES))
        to_partner(o).start()

    def pass_on(o):
        to_partner(o).wait_recv()
        pbuf[o] = sbuf[o, core] + prec[o]

    source_sums(1)

    def source_step(o, _):
        source_sums(lax.rem(o + 1, G))
        pass_on(o)
        to_owner(o).start()
        return 0

    lax.fori_loop(1, G, source_step, 0)
    pass_on(0)

    finish(wcopies)
    total = wbuf[me_s] + sum(wrec[o] for o in range(S - 1))
    tbuf[...] = total[0:dims] / total[dims:dims + 1]
    tcopies = to_column(tbuf, trec, tsend, trecv)
    begin(tcopies)
    to_ref[:, span(me_s, QW)] = tbuf[...]

    def settle(o, acc):
        to_owner(o).wait()
        return acc + srec[o - 1]

    total = lax.fori_loop(1, G, settle, pbuf[0])
    so_ref[...] = total[0:dims] / total[dims:dims + 1]

    def sent(o, _):
        to_partner(o).wait_send()
        return 0

    lax.fori_loop(0, G, sent, 0)
    finish(tcopies)
    for o in range(1, S):
        to_ref[:, span(lax.rem(me_s + S - o, S), QW)] = trec[o - 1]


def shards(S, T, source_pca, target_pca, source_labels, target_labels, block_mask):
    dims, R = source_pca.shape
    C = target_pca.shape[1]
    G = T // 2
    CB, RB = C // LANES, R // LANES
    vmem = pltpu.VMEM
    dma = pltpu.SemaphoreType.DMA
    whole = pl.BlockSpec(memory_space=pltpu.VMEM)
    return pl.pallas_call(
        functools.partial(kernel, S, T),
        out_shape=(jax.ShapeDtypeStruct((dims, R // T), F32), jax.ShapeDtypeStruct((dims, C), F32)),
        in_specs=[whole] * 5,
        out_specs=(whole, whole),
        scratch_shapes=[
            vmem((8 * dims, R), BF16), vmem((C, 8 * dims), BF16), vmem((C, R), F32),
            vmem((C, R), BF16), vmem((C, R), BF16), vmem((GROUP, R), F32),
            vmem((C, LANES), F32), vmem((C, LANES), F32), vmem((C, LANES), F32),
            vmem((C, LANES), F32),
            vmem((2 * dims + 2 * GROUP, R), BF16), vmem((2 * dims + 2 * GROUP, C), BF16),
            vmem((RB, LANES), F32), vmem((G - 1, RB, LANES), F32), vmem((RB, LANES), F32),
            vmem((RB, LANES), F32),
            vmem((CB, LANES), F32), vmem((CB, LANES), F32), vmem((S - 1, CB, LANES), F32),
            vmem((RB, LANES), F32), vmem((G - 1, RB, LANES), F32), vmem((RB, LANES), F32),
            vmem((RB, LANES), F32),
            vmem((CB, LANES), F32), vmem((S - 1, CB, LANES), F32),
            vmem((S, PAD, C // S), F32), vmem((S - 1, PAD, C // S), F32),
            vmem((dims, C // S), F32), vmem((S - 1, dims, C // S), F32),
            vmem((G, 2, PAD, LANES), F32), vmem((G, PAD, LANES), F32), vmem((G, PAD, LANES), F32),
            vmem((G - 1, PAD, LANES), F32),
            dma((G - 1,)), dma((G - 1,)), dma, dma, dma((S - 1,)), dma((S - 1,)),
            dma((G - 1,)), dma((G - 1,)), dma, dma, dma((S - 1,)), dma((S - 1,)),
            dma((S - 1,)), dma((S - 1,)), dma((S - 1,)), dma((S - 1,)),
            dma((G,)), dma((G,)), dma((G - 1,)), dma((G - 1,)),
        ],
        compiler_params=pltpu.CompilerParams(
            collective_id=0, has_side_effects=True, vmem_limit_bytes=60 * 2**20),
    )(source_pca, target_pca, source_labels.reshape(1, R), target_labels.reshape(1, C), block_mask)


def solution(mesh):
    placed = (P(None, "src"), P(None, "tgt"), P("src"), P("tgt"), P())
    return jax.shard_map(
        functools.partial(shards, mesh.shape["src"], mesh.shape["tgt"]),
        mesh=mesh,
        in_specs=placed,
        out_specs=(P(None, ("src", "tgt")), P(None, "tgt")),
        check_vma=False,
    )
```

```python
import functools
import math

import jax
import jax.numpy as jnp
from jax import lax
from jax.experimental import pallas as pl
from jax.experimental.pallas import tpu as pltpu
from jax.sharding import PartitionSpec as P

ITERS = 2
EPSILON = 0.05
BARRED = -(2.0**100)
MESH = pl.DeviceIdType.MESH
F32 = jnp.float32
BF16 = jnp.bfloat16
LANES = 128
GROUP = 8
PAD = 72


def in_three(value):
    first = value.astype(BF16)
    rest = value - first.astype(F32)
    second = rest.astype(BF16)
    third = (rest - second.astype(F32)).astype(BF16)
    return first, second, third


def in_two(value):
    first = value.astype(BF16)
    return first, (value - first.astype(F32)).astype(BF16)


def turned(row):
    return jnp.broadcast_to(row, (LANES, LANES)).T


def lse_of(parts):
    top = functools.reduce(jnp.maximum, parts)
    return top + jnp.log2(sum(jnp.exp2(p - top) for p in parts))


def span(index, size):
    return pl.ds(pl.multiple_of(index * size, size), size)


def kernel(S, T, x_ref, y_ref, sl_ref, tl_ref, mask_ref, so_ref, to_ref,
           xa, ya, zr, ehi, elo, frow, mp, mb, sp, sb, xw, yw,
           lbuf, lrec, lpair, lown, lprec, mbuf, gbuf, grec,
           rbuf, rrec, rpair, rown, rprec, cbuf, crec,
           wbuf, wrec, tbuf, trec, sbuf, prec, pbuf, srec,
           lsend, lrecv, psend, precv, gsend, grecv,
           rsend, rrecv, qsend, qrecv, csend, crecv,
           wsend, wrecv, tsend, trecv, bsend, brecv, ssend, srecv):
    dims, R = x_ref.shape
    C = y_ref.shape[1]
    G = T // 2
    QW = C // S
    CB = C // LANES
    RB = R // LANES
    scale = math.log2(math.e) / (EPSILON * dims)
    me_s, me_t = lax.axis_index("src"), lax.axis_index("tgt")
    core = lax.rem(me_t, 2)
    chip = me_t // 2
    partner = me_t + 1 - 2 * core

    def mate(o):
        return (me_s, lax.rem(me_t + 2 * o, T))

    def above(o):
        return (lax.rem(me_s + o, S), me_t)

    pair = (me_s, partner)
    everyone = [mate(o) for o in range(1, G)] + [above(o) for o in range(1, S)] + [pair]
    barrier = pltpu.get_barrier_semaphore()
    for device in everyone:
        pl.semaphore_signal(barrier, inc=1, device_id=device, device_id_type=MESH)

    def remote(src, dst, send, recv, device):
        return pltpu.make_async_remote_copy(
            src_ref=src, dst_ref=dst, send_sem=send, recv_sem=recv,
            device_id=device, device_id_type=MESH)

    def to_mates(src, dst, send, recv):
        return [remote(src, dst.at[o - 1], send.at[o - 1], recv.at[o - 1], mate(o))
                for o in range(1, G)]

    def to_column(src, dst, send, recv):
        return [remote(src, dst.at[o - 1], send.at[o - 1], recv.at[o - 1], above(o))
                for o in range(1, S)]

    def begin(copies):
        for copy in copies:
            copy.start()

    def finish(copies):
        for copy in copies:
            copy.wait()

    def chunks(q):
        return slice(q * LANES, (q + 1) * LANES)

    XC = min(512, R // 2)

    half = R // 2
    half_rows = RB // 2

    def natural(slot):
        return slot + core - 2 * slot * core

    def prepare_source(c, _):
        at = span(c, XC)
        place = natural(c // (half // XC)) * half + lax.rem(c, half // XC) * XC
        place = pl.ds(pl.multiple_of(place, XC), XC)
        x = x_ref[:, place]
        x1, x2, x3 = in_three(x)
        for k, part in enumerate((x1, x2, x1, x2, x3, x1)):
            xa[k * dims:(k + 1) * dims, at] = part
        ids = lax.broadcasted_iota(jnp.int32, (dims, XC), 0)
        xa[6 * dims:7 * dims, at] = jnp.where(ids == sl_ref[:, place], 1.0, 0.0).astype(BF16)
        n1, n2, n3 = (p.astype(F32) for p in in_three(-scale * jnp.sum(x * x, 0, keepdims=True)))
        norm = jnp.where(ids == 3, n1, jnp.where(ids == 4, n2, jnp.where(ids == 5, n3, 0.0)))
        xa[7 * dims:8 * dims, at] = jnp.where(ids < 3, 1.0, norm).astype(BF16)
        return 0

    lax.fori_loop(0, R // XC, prepare_source, 0)

    y = y_ref[...]
    y1, y2, y3 = (p.astype(F32) for p in in_three(2.0 * scale * y))
    ids = lax.broadcasted_iota(jnp.int32, (dims, C), 0)
    onehot = jnp.where(ids == tl_ref[...], 1.0, 0.0).astype(BF16)
    allowed = jnp.dot(mask_ref[...].astype(F32).astype(BF16), onehot, preferred_element_type=F32)
    penalty = jnp.where(allowed > 0.5, 0.0, BARRED)
    n1, n2, n3 = (p.astype(F32) for p in in_three(-scale * jnp.sum(y * y, 0, keepdims=True)))
    norm = jnp.where(ids == 0, n1, jnp.where(ids == 1, n2, jnp.where(ids == 2, n3, 0.0)))
    norm = jnp.where((ids >= 3) & (ids < 6), 1.0, norm)
    for k, (a, b) in enumerate(((y1, y1), (y2, y2), (y1, y3), (penalty, norm))):
        ya[:, k * LANES:(k + 1) * LANES] = jnp.concatenate([a, b], 0).T.astype(BF16)

    block = 2 * LANES
    sub = 8 * GROUP

    def first_rows(slot):
        behind = None
        for u in range(half // block + 1):
            ahead = None
            if u < half // block:
                at = slice(slot * half + u * block, slot * half + (u + 1) * block)
                z = jnp.dot(ya[...], xa[:, at], preferred_element_type=F32)
                zr[:, at] = z
                tops = functools.reduce(
                    jnp.maximum, [z[k * sub:(k + 1) * sub] for k in range(C // sub)])
                ahead = at, jnp.max(tops, 0, keepdims=True)
            if behind is not None:
                at, top = behind
                total = sum(
                    jnp.exp2(zr[k * sub:(k + 1) * sub, at] - top) for k in range(C // sub))
                lse = top + jnp.log2(jnp.sum(total, 0, keepdims=True))
                for k in range(2):
                    lbuf[slot, 2 * (u - 1) + k:2 * (u - 1) + k + 1, :] = lse[:, chunks(k)]
            behind = ahead

    first_rows(1)
    pl.semaphore_wait(barrier, len(everyone))
    early = remote(lbuf.at[1], lprec.at[0], psend.at[0], precv.at[0], pair)
    early.start()
    first_rows(0)
    early.wait()
    lpair[...] = lse_of([lbuf[0], lprec[0]])
    copies = to_mates(lpair, lrec, lsend, lrecv)
    begin(copies)
    finish(copies)
    lown[...] = -math.log2(R * S) - lse_of([lpair[...]] + [lrec[o] for o in range(G - 1)])
    late = remote(lown, lprec.at[1], psend.at[1], precv.at[1], pair)
    late.start()

    def lanes_of(slot, q):
        return slice(slot * half + q * LANES, slot * half + (q + 1) * LANES)

    def spread(slot, value):
        for q in range(half_rows):
            frow[:, lanes_of(slot, q)] = jnp.broadcast_to(value[q:q + 1, :], (GROUP, LANES))

    WIDE = 4

    def parts_of(value):
        return [value[g * GROUP:(g + 1) * GROUP] for g in range(value.shape[0] // GROUP)]

    def by_rows(slot, step, combine, into, more):

        def body(j, _):
            at = span(j, WIDE * GROUP)
            acc = [[None, None] for _ in range(WIDE)]
            for q in range(half_rows):
                row = frow[:, lanes_of(slot, q)]
                for g, z in enumerate(parts_of(zr[at, lanes_of(slot, q)])):
                    value = step(z, row)
                    old = acc[g][q % 2]
                    acc[g][q % 2] = value if old is None else combine(old, value)
            value = jnp.concatenate([combine(*pair_) for pair_ in acc], 0)
            into[at, :] = combine(into[at, :], value) if more else value
            return 0

        lax.fori_loop(0, C // (WIDE * GROUP), body, 0)

    spread(0, lown[...])
    by_rows(0, jnp.add, jnp.maximum, mp, False)
    late.wait()
    spread(1, lprec[1])
    by_rows(1, jnp.add, jnp.maximum, mp, True)

    for b in range(CB):
        rows = slice(b * LANES, (b + 1) * LANES)
        top = jnp.max(mp[rows, :].T, 0, keepdims=True)
        mbuf[b:b + 1, :] = top
        mb[rows, :] = turned(top)

    def weigh(j, _):
        at = span(j, 2 * GROUP)
        peak = mb[at, :]
        acc = [None, None]
        for q in range(RB):
            row = jnp.concatenate([frow[:, chunks(q)]] * 2, 0)
            e = jnp.exp2(zr[at, chunks(q)] + row - peak)
            zr[at, chunks(q)] = e
            acc[q % 2] = e if acc[q % 2] is None else acc[q % 2] + e
        sp[at, :] = acc[0] + acc[1]
        return 0

    lax.fori_loop(0, C // (2 * GROUP), weigh, 0)
    for b in range(CB):
        rows = slice(b * LANES, (b + 1) * LANES)
        total = jnp.sum(sp[rows, :].T, 0, keepdims=True)
        gbuf[b:b + 1, :] = mbuf[b:b + 1, :] + jnp.log2(total)

    copies = to_column(gbuf, grec, gsend, grecv)
    begin(copies)

    def halve(j, _):
        at = span(j, 2 * GROUP)
        ehi[at, :], elo[at, :] = in_two(zr[at, :])
        return 0

    lax.fori_loop(0, C // (2 * GROUP), halve, 0)
    finish(copies)
    lse = lse_of([gbuf[...]] + [grec[o] for o in range(S - 1)])
    sig = jnp.exp2(mbuf[...] - lse)
    for b in range(CB):
        sb[b * LANES:(b + 1) * LANES, :] = turned(sig[b:b + 1, :])

    def row_mass(slot):

        def body(j, acc):
            at = span(j, WIDE * GROUP)
            acc = list(acc)
            weights = parts_of(sb[at, :])
            for q in range(half_rows):
                terms = [z * w for z, w in zip(parts_of(zr[at, lanes_of(slot, q)]), weights)]
                acc[q] = acc[q] + ((terms[0] + terms[1]) + (terms[2] + terms[3]))
            return tuple(acc)

        zero = jnp.zeros((GROUP, LANES), F32)
        acc = lax.fori_loop(0, C // (WIDE * GROUP), body, (zero,) * half_rows)
        for q, part in enumerate(acc):
            rbuf[slot, q:q + 1, :] = jnp.sum(part, 0, keepdims=True)

    row_mass(1)
    early = remote(rbuf.at[1], rprec.at[0], qsend.at[0], qrecv.at[0], pair)
    early.start()
    row_mass(0)
    early.wait()
    rpair[...] = rbuf[0] + rprec[0]
    copies = to_mates(rpair, rrec, rsend, rrecv)
    begin(copies)
    finish(copies)
    rown[...] = (C * T / (R * S)) / (rpair[...] + sum(rrec[o] for o in range(G - 1)))
    late = remote(rown, rprec.at[1], qsend.at[1], qrecv.at[1], pair)
    late.start()
    spread(0, rown[...])
    by_rows(0, jnp.multiply, jnp.add, sp, False)
    late.wait()
    spread(1, rprec[1])
    by_rows(1, jnp.multiply, jnp.add, sp, True)
    for b in range(CB):
        rows = slice(b * LANES, (b + 1) * LANES)
        cbuf[b:b + 1, :] = sig[b:b + 1, :] * jnp.sum(sp[rows, :].T, 0, keepdims=True)
    copies = to_column(cbuf, crec, csend, crecv)
    begin(copies)

    tail = lax.broadcasted_iota(jnp.int32, (2 * GROUP, LANES), 0)

    def with_mass(dst, at, value, mass):
        hi, lo = in_two(value)
        dst[0:dims, at] = hi
        dst[dims:2 * dims, at] = lo
        m1, m2 = (p.astype(F32) for p in in_two(mass))
        dst[2 * dims:2 * dims + 2 * GROUP, at] = jnp.where(
            tail == 0, m1, jnp.where(tail == 1, m2, 0.0)).astype(BF16)

    for q in range(RB):
        row = frow[0:1, chunks(q)]
        place = natural(q // half_rows) * half + (q % half_rows) * LANES
        place = pl.ds(pl.multiple_of(place, LANES), LANES)
        with_mass(xw, chunks(q), x_ref[:, place] * row, row)

    def folded(out):
        value = out[0:dims] + out[dims:2 * dims]
        mass = jnp.sum(out[2 * dims:], 0, keepdims=True)
        return value, mass

    across = (((1,), (1,)), ((), ()))

    for k in range(S):
        at = slice(k * QW, (k + 1) * QW)
        value, mass = folded(
            lax.dot_general(xw[...], ehi[at, :], across, preferred_element_type=F32)
            + lax.dot_general(xw[...], elo[at, :], across, preferred_element_type=F32))
        for b in range(QW // LANES):
            row = sig[k * (QW // LANES) + b:k * (QW // LANES) + b + 1, :]
            wbuf[k, 0:dims, chunks(b)] = value[:, chunks(b)] * row
            wbuf[k, dims:PAD, chunks(b)] = jnp.broadcast_to(
                mass[:, chunks(b)] * row, (PAD - dims, LANES))
    wcopies = [
        remote(wbuf.at[lax.rem(me_s + o, S)], wrec.at[o - 1], wsend.at[o - 1], wrecv.at[o - 1],
               above(o)) for o in range(1, S)]
    begin(wcopies)
    finish(copies)
    factor = sig / (cbuf[...] + sum(crec[o] for o in range(S - 1)))
    for b in range(CB):
        row = factor[b:b + 1, :]
        with_mass(yw, chunks(b), y_ref[:, chunks(b)] * row, row)

    def to_partner(o):
        return remote(sbuf.at[o, 1 - core], prec.at[o], bsend.at[o], brecv.at[o], pair)

    def to_owner(o):
        return remote(pbuf.at[o], srec.at[o - 1], ssend.at[o - 1], srecv.at[o - 1], mate(o))

    def source_sums(o):
        owner = lax.rem(chip + o, G)
        place = natural(owner // (G // 2)) * half + lax.rem(owner, G // 2) * (2 * LANES)
        at = pl.ds(pl.multiple_of(place, 2 * LANES), 2 * LANES)
        value, mass = folded(
            jnp.dot(yw[...], ehi[:, at], preferred_element_type=F32)
            + jnp.dot(yw[...], elo[:, at], preferred_element_type=F32))
        for k in range(2):
            sbuf[o, k, 0:dims, :] = value[:, chunks(k)]
            sbuf[o, k, dims:PAD, :] = jnp.broadcast_to(mass[:, chunks(k)], (PAD - dims, LANES))

    def pass_on(o):
        to_partner(o).wait_recv()
        pbuf[o] = sbuf[o, core] + prec[o]

    V = min(4, G)

    def compute(g):
        for v in range(V):
            source_sums(lax.rem(g * V + v + 1, G))
        for v in range(V):
            to_partner(lax.rem(g * V + v + 1, G)).start()

    def relay(g):
        for v in range(V):
            pass_on(g * V + v + 1)
            to_owner(g * V + v + 1).start()

    compute(0)

    def source_step(g, _):
        compute(g + 1)
        relay(g)
        return 0

    lax.fori_loop(0, G // V - 1, source_step, 0)
    for v in range(G - V + 1, G):
        pass_on(v)
        to_owner(v).start()
    pass_on(0)

    finish(wcopies)
    total = wbuf[me_s] + sum(wrec[o] for o in range(S - 1))
    tbuf[...] = total[0:dims] / total[dims:dims + 1]
    tcopies = to_column(tbuf, trec, tsend, trecv)
    begin(tcopies)
    to_ref[:, span(me_s, QW)] = tbuf[...]

    def settle(o, acc):
        to_owner(o).wait()
        return acc + srec[o - 1]

    total = lax.fori_loop(1, G, settle, pbuf[0])
    so_ref[...] = total[0:dims] / total[dims:dims + 1]

    def sent(o, _):
        to_partner(o).wait_send()
        return 0

    lax.fori_loop(0, G, sent, 0)
    finish(tcopies)
    for o in range(1, S):
        to_ref[:, span(lax.rem(me_s + S - o, S), QW)] = trec[o - 1]


def shards(S, T, source_pca, target_pca, source_labels, target_labels, block_mask):
    dims, R = source_pca.shape
    C = target_pca.shape[1]
    G = T // 2
    CB, RB = C // LANES, R // LANES
    vmem = pltpu.VMEM
    dma = pltpu.SemaphoreType.DMA
    whole = pl.BlockSpec(memory_space=pltpu.VMEM)
    return pl.pallas_call(
        functools.partial(kernel, S, T),
        out_shape=(jax.ShapeDtypeStruct((dims, R // T), F32), jax.ShapeDtypeStruct((dims, C), F32)),
        in_specs=[whole] * 5,
        out_specs=(whole, whole),
        scratch_shapes=[
            vmem((8 * dims, R), BF16), vmem((C, 8 * dims), BF16), vmem((C, R), F32),
            vmem((C, R), BF16), vmem((C, R), BF16), vmem((GROUP, R), F32),
            vmem((C, LANES), F32), vmem((C, LANES), F32), vmem((C, LANES), F32),
            vmem((C, LANES), F32),
            vmem((2 * dims + 2 * GROUP, R), BF16), vmem((2 * dims + 2 * GROUP, C), BF16),
            vmem((2, RB // 2, LANES), F32), vmem((G - 1, RB // 2, LANES), F32),
            vmem((RB // 2, LANES), F32), vmem((RB // 2, LANES), F32), vmem((2, RB // 2, LANES), F32),
            vmem((CB, LANES), F32), vmem((CB, LANES), F32), vmem((S - 1, CB, LANES), F32),
            vmem((2, RB // 2, LANES), F32), vmem((G - 1, RB // 2, LANES), F32),
            vmem((RB // 2, LANES), F32), vmem((RB // 2, LANES), F32), vmem((2, RB // 2, LANES), F32),
            vmem((CB, LANES), F32), vmem((S - 1, CB, LANES), F32),
            vmem((S, PAD, C // S), F32), vmem((S - 1, PAD, C // S), F32),
            vmem((dims, C // S), F32), vmem((S - 1, dims, C // S), F32),
            vmem((G, 2, PAD, LANES), F32), vmem((G, PAD, LANES), F32), vmem((G, PAD, LANES), F32),
            vmem((G - 1, PAD, LANES), F32),
            dma((G - 1,)), dma((G - 1,)), dma((2,)), dma((2,)), dma((S - 1,)), dma((S - 1,)),
            dma((G - 1,)), dma((G - 1,)), dma((2,)), dma((2,)), dma((S - 1,)), dma((S - 1,)),
            dma((S - 1,)), dma((S - 1,)), dma((S - 1,)), dma((S - 1,)),
            dma((G,)), dma((G,)), dma((G - 1,)), dma((G - 1,)),
        ],
        compiler_params=pltpu.CompilerParams(
            collective_id=0, has_side_effects=True, vmem_limit_bytes=60 * 2**20),
    )(source_pca, target_pca, source_labels.reshape(1, R), target_labels.reshape(1, C), block_mask)


def solution(mesh):
    placed = (P(None, "src"), P(None, "tgt"), P("src"), P("tgt"), P())
    return jax.shard_map(
        functools.partial(shards, mesh.shape["src"], mesh.shape["tgt"]),
        mesh=mesh,
        in_specs=placed,
        out_specs=(P(None, ("src", "tgt")), P(None, "tgt")),
        check_vma=False,
    )
```

```python
import functools
import math

import jax
import jax.numpy as jnp
from jax import lax
from jax.experimental import pallas as pl
from jax.experimental.pallas import tpu as pltpu
from jax.sharding import PartitionSpec as P

ITERS = 2
EPSILON = 0.05
BARRED = -(2.0**100)
MESH = pl.DeviceIdType.MESH
F32 = jnp.float32
BF16 = jnp.bfloat16
LANES = 128
GROUP = 8
PAD = 72


def in_two(value):
    first = value.astype(BF16)
    return first, (value - first.astype(F32)).astype(BF16)


def turned(row):
    return jnp.broadcast_to(row, (LANES, LANES)).T


def lse_of(parts):
    top = functools.reduce(jnp.maximum, parts)
    return top + jnp.log2(sum(jnp.exp2(p - top) for p in parts))


def span(index, size):
    return pl.ds(pl.multiple_of(index * size, size), size)


def kernel(S, T, x_hbm, y_ref, sl_ref, tl_ref, mask_ref, so_ref, to_ref,
           x_ref, nbuf, fetched, xa, ya, zr, ehi, elo, frow, mp, mb, sp, sb, xw, yw,
           lbuf, lrec, lpair, lown, lprec, mbuf, gbuf, grec,
           rbuf, rrec, rpair, rown, rprec, cbuf, crec,
           wbuf, wrec, tbuf, trec, sbuf, prec, pbuf, srec,
           lsend, lrecv, psend, precv, gsend, grecv,
           rsend, rrecv, qsend, qrecv, csend, crecv,
           wsend, wrecv, tsend, trecv, bsend, brecv, ssend, srecv):
    dims, R = x_ref.shape
    C = y_ref.shape[1]
    G = T // 2
    QW = C // S
    CB = C // LANES
    RB = R // LANES
    scale = math.log2(math.e) / (EPSILON * dims)
    me_s, me_t = lax.axis_index("src"), lax.axis_index("tgt")
    core = lax.rem(me_t, 2)
    chip = me_t // 2
    partner = me_t + 1 - 2 * core

    GZ = min(4, G)
    GX = G // GZ
    offsets = sorted(
        ((dx, dz) for dx in range(GX) for dz in range(GZ)),
        key=lambda d: min(d[0], GX - d[0]) + min(d[1], GZ - d[1]))
    offsets = offsets[:1] + offsets[:0:-1]

    def chip_at(o):
        dx, dz = offsets[o]
        return lax.rem(chip // GZ + dx, GX) * GZ + lax.rem(lax.rem(chip, GZ) + dz, GZ)

    def mate(o):
        return (me_s, 2 * chip_at(o) + core)

    def above(o):
        return (lax.rem(me_s + o, S), me_t)

    pair = (me_s, partner)
    everyone = [mate(o) for o in range(1, G)] + [above(o) for o in range(1, S)] + [pair]
    barrier = pltpu.get_barrier_semaphore()
    for device in everyone:
        pl.semaphore_signal(barrier, inc=1, device_id=device, device_id_type=MESH)

    def remote(src, dst, send, recv, device):
        return pltpu.make_async_remote_copy(
            src_ref=src, dst_ref=dst, send_sem=send, recv_sem=recv,
            device_id=device, device_id_type=MESH)

    def to_mates(src, dst, send, recv):
        return [remote(src, dst.at[o - 1], send.at[o - 1], recv.at[o - 1], mate(o))
                for o in range(1, G)]

    def to_column(src, dst, send, recv):
        return [remote(src, dst.at[o - 1], send.at[o - 1], recv.at[o - 1], above(o))
                for o in range(1, S)]

    def begin(copies):
        for copy in copies:
            copy.start()

    def finish(copies):
        for copy in copies:
            copy.wait()

    def chunks(q):
        return slice(q * LANES, (q + 1) * LANES)

    XC = min(512, R // 2)

    half = R // 2
    half_rows = RB // 2

    def natural(slot):
        return slot + core - 2 * slot * core

    def source_place(c):
        place = natural(c // (half // XC)) * half + lax.rem(c, half // XC) * XC
        return pl.ds(pl.multiple_of(place, XC), XC)

    def fetch(c):
        place = source_place(c)
        return pltpu.make_async_copy(x_hbm.at[:, place], x_ref.at[:, place], fetched.at[c])

    for c in range(R // XC):
        fetch(c).start()

    def prepare_source(c, _):
        at = span(c, XC)
        place = source_place(c)
        fetch(c).wait()
        x = x_ref[:, place]
        x1, x2 = in_two(x)
        for k, part in enumerate((x1, x2, x1)):
            xa[k * dims:(k + 1) * dims, at] = part
        ids = lax.broadcasted_iota(jnp.int32, (dims, XC), 0)
        xa[3 * dims:, at] = jnp.where(ids == sl_ref[:, place], 1.0, 0.0).astype(BF16)
        norm = -scale * jnp.sum(x * x, 0, keepdims=True)
        for k in range(XC // LANES):
            nbuf[pl.ds(c * (XC // LANES) + k, 1), :] = norm[:, chunks(k)]
        return 0

    y = y_ref[...]
    y1, y2 = (p.astype(F32) for p in in_two(2.0 * scale * y))
    ids = lax.broadcasted_iota(jnp.int32, (dims, C), 0)
    onehot = jnp.where(ids == tl_ref[...], 1.0, 0.0).astype(BF16)
    allowed = jnp.dot(mask_ref[...].astype(F32).astype(BF16), onehot, preferred_element_type=F32)
    penalty = jnp.where(allowed > 0.5, 0.0, BARRED)
    for k, (a, b) in enumerate(((y1, y1), (y2, penalty))):
        ya[:, k * LANES:(k + 1) * LANES] = jnp.concatenate([a, b], 0).T.astype(BF16)
    norm = -scale * jnp.sum(y * y, 0, keepdims=True)
    for b in range(CB):
        mb[b * LANES:(b + 1) * LANES, :] = turned(norm[:, chunks(b)])
    lax.fori_loop(0, R // XC, prepare_source, 0)

    block = 2 * LANES
    sub = 16 * GROUP

    def first_rows(slot):
        behind = None
        for u in range(half // block + 1):
            ahead = None
            if u < half // block:
                at = slice(slot * half + u * block, slot * half + (u + 1) * block)
                z = jnp.dot(ya[...], xa[:, at], preferred_element_type=F32)
                ahead = []
                for k in range(2):
                    tops = None
                    for i in range(C // sub):
                        rows = slice(i * sub, (i + 1) * sub)
                        part = z[rows, chunks(k)] + mb[rows, :]
                        zr[slot * half_rows + 2 * u + k, rows, :] = part
                        tops = part if tops is None else jnp.maximum(tops, part)
                    ahead.append(jnp.max(tops, 0, keepdims=True))
            if behind is not None:
                for k in range(2):
                    row, top = 2 * (u - 1) + k, behind[k]
                    total = sum(
                        jnp.exp2(zr[slot * half_rows + row, i * sub:(i + 1) * sub, :] - top)
                        for i in range(C // sub))
                    lbuf[slot, row:row + 1, :] = top + jnp.log2(jnp.sum(total, 0, keepdims=True))
            behind = ahead

    first_rows(1)
    pl.semaphore_wait(barrier, len(everyone))
    early = remote(lbuf.at[1], lprec.at[0], psend.at[0], precv.at[0], pair)
    early.start()
    first_rows(0)
    early.wait()
    lpair[...] = lse_of([lbuf[0], lprec[0]])
    copies = to_mates(lpair, lrec, lsend, lrecv)
    begin(copies)
    finish(copies)
    lown[...] = -math.log2(R * S) - (
        lse_of([lpair[...]] + [lrec[o] for o in range(G - 1)]) + nbuf[0:half_rows, :])
    late = remote(lown, lprec.at[1], psend.at[1], precv.at[1], pair)
    late.start()

    def lanes_of(slot, q):
        return slice(slot * half + q * LANES, slot * half + (q + 1) * LANES)

    def spread(slot, value):
        for q in range(half_rows):
            frow[:, lanes_of(slot, q)] = jnp.broadcast_to(value[q:q + 1, :], (GROUP, LANES))

    WIDE = 4

    def parts_of(value):
        return [value[g * GROUP:(g + 1) * GROUP] for g in range(value.shape[0] // GROUP)]

    def by_rows(slot, step, combine, into, more):

        def body(j, _):
            at = span(j, WIDE * GROUP)
            acc = [[None, None] for _ in range(WIDE)]
            for q in range(half_rows):
                row = frow[:, lanes_of(slot, q)]
                for g, z in enumerate(parts_of(zr[slot * half_rows + q, at, :])):
                    value = step(z, row)
                    old = acc[g][q % 2]
                    acc[g][q % 2] = value if old is None else combine(old, value)
            value = jnp.concatenate([combine(*pair_) for pair_ in acc], 0)
            into[at, :] = combine(into[at, :], value) if more else value
            return 0

        lax.fori_loop(0, C // (WIDE * GROUP), body, 0)

    spread(0, lown[...] + nbuf[0:half_rows, :])
    by_rows(0, jnp.add, jnp.maximum, mp, False)
    late.wait()
    spread(1, lprec[1] + nbuf[half_rows:, :])
    by_rows(1, jnp.add, jnp.maximum, mp, True)

    for b in range(CB):
        rows = slice(b * LANES, (b + 1) * LANES)
        top = jnp.max(mp[rows, :].T, 0, keepdims=True)
        mbuf[b:b + 1, :] = top
        mb[rows, :] = turned(top)

    def weigh(j, _):
        at = span(j, WIDE * GROUP)
        peak = mb[at, :]
        acc = [None, None]
        for q in range(RB):
            row = jnp.concatenate([frow[:, chunks(q)]] * WIDE, 0)
            e = jnp.exp2(zr[q, at, :] + row - peak)
            zr[q, at, :] = e
            acc[q % 2] = e if acc[q % 2] is None else acc[q % 2] + e
        sp[at, :] = acc[0] + acc[1]
        return 0

    lax.fori_loop(0, C // (WIDE * GROUP), weigh, 0)
    for b in range(CB):
        rows = slice(b * LANES, (b + 1) * LANES)
        total = jnp.sum(sp[rows, :].T, 0, keepdims=True)
        gbuf[b:b + 1, :] = mbuf[b:b + 1, :] + jnp.log2(total)

    copies = to_column(gbuf, grec, gsend, grecv)
    begin(copies)

    def halve(j, _):
        at = span(j, 4 * GROUP)
        for q in range(RB):
            ehi[q, at, :], elo[q, at, :] = in_two(zr[q, at, :])
        return 0

    lax.fori_loop(0, C // (4 * GROUP), halve, 0)
    finish(copies)
    lse = lse_of([gbuf[...]] + [grec[o] for o in range(S - 1)])
    sig = jnp.exp2(mbuf[...] - lse)
    mbuf[...] = sig
    for b in range(CB):
        sb[b * LANES:(b + 1) * LANES, :] = turned(sig[b:b + 1, :])

    def row_mass(slot):

        def body(j, acc):
            at = span(j, WIDE * GROUP)
            acc = list(acc)
            weights = parts_of(sb[at, :])
            for q in range(half_rows):
                terms = [z * w for z, w in zip(parts_of(zr[slot * half_rows + q, at, :]), weights)]
                acc[q] = acc[q] + ((terms[0] + terms[1]) + (terms[2] + terms[3]))
            return tuple(acc)

        zero = jnp.zeros((GROUP, LANES), F32)
        acc = lax.fori_loop(0, C // (WIDE * GROUP), body, (zero,) * half_rows)
        for q, part in enumerate(acc):
            rbuf[slot, q:q + 1, :] = jnp.sum(part, 0, keepdims=True)

    row_mass(1)
    early = remote(rbuf.at[1], rprec.at[0], qsend.at[0], qrecv.at[0], pair)
    early.start()
    row_mass(0)
    early.wait()
    rpair[...] = rbuf[0] + rprec[0]
    copies = to_mates(rpair, rrec, rsend, rrecv)
    begin(copies)
    finish(copies)
    rown[...] = (C * T / (R * S)) / (rpair[...] + sum(rrec[o] for o in range(G - 1)))
    late = remote(rown, rprec.at[1], qsend.at[1], qrecv.at[1], pair)
    late.start()
    spread(0, rown[...])
    by_rows(0, jnp.multiply, jnp.add, sp, False)
    late.wait()
    spread(1, rprec[1])
    by_rows(1, jnp.multiply, jnp.add, sp, True)
    for b in range(CB):
        rows = slice(b * LANES, (b + 1) * LANES)
        cbuf[b:b + 1, :] = sig[b:b + 1, :] * jnp.sum(sp[rows, :].T, 0, keepdims=True)
    copies = to_column(cbuf, crec, csend, crecv)
    begin(copies)

    tail = lax.broadcasted_iota(jnp.int32, (2 * GROUP, LANES), 0)

    def with_mass(dst, at, value, mass):
        hi, lo = in_two(value)
        dst[0:dims, at] = hi
        dst[dims:2 * dims, at] = lo
        m1, m2 = (p.astype(F32) for p in in_two(mass))
        dst[2 * dims:2 * dims + 2 * GROUP, at] = jnp.where(
            tail == 0, m1, jnp.where(tail == 1, m2, 0.0)).astype(BF16)

    for q in range(RB):
        row = frow[0:1, chunks(q)]
        place = natural(q // half_rows) * half + (q % half_rows) * LANES
        place = pl.ds(pl.multiple_of(place, LANES), LANES)
        with_mass(xw, chunks(q), x_ref[:, place] * row, row)

    def folded(out):
        value = out[0:dims] + out[dims:2 * dims]
        mass = jnp.sum(out[2 * dims:], 0, keepdims=True)
        return value, mass

    across = (((1,), (1,)), ((), ()))

    def sent_target(o):
        return remote(wbuf.at[o], wrec.at[o - 1], wsend.at[o - 1], wrecv.at[o - 1], above(o))

    def target_sums(which):
        owners = [lax.rem(me_s + o, S) for o in which]
        outs = [None] * len(which)
        depth = min(8, RB)
        for k in range(0, RB, depth):
            left = xw[:, k * LANES:(k + depth) * LANES]
            for ref in (ehi, elo):
                for i, owner in enumerate(owners):
                    at = span(owner, QW)
                    right = jnp.concatenate([ref[q, at, :] for q in range(k, k + depth)], 1)
                    part = lax.dot_general(left, right, across, preferred_element_type=F32)
                    outs[i] = part if outs[i] is None else outs[i] + part
        for o, owner, out in zip(which, owners, outs):
            value, mass = folded(out)
            for b in range(QW // LANES):
                row = mbuf[pl.ds(owner * (QW // LANES) + b, 1), :]
                wbuf[o, 0:dims, chunks(b)] = value[:, chunks(b)] * row
                wbuf[o, dims:PAD, chunks(b)] = jnp.broadcast_to(
                    mass[:, chunks(b)] * row, (PAD - dims, LANES))
        for o in which:
            if o:
                sent_target(o).start()

    def to_partner(o):
        return remote(sbuf.at[o, 1 - core], prec.at[o], bsend.at[o], brecv.at[o], pair)

    def to_owner(o):
        return remote(pbuf.at[o], srec.at[o - 1], ssend.at[o - 1], srecv.at[o - 1], mate(o))

    def source_sums(o):
        owner = chip_at(o)
        place = natural(owner // (G // 2)) * half_rows + lax.rem(owner, G // 2) * 2

        def wide(ref):
            return jnp.concatenate([ref[place], ref[place + 1]], 1)

        value, mass = folded(
            jnp.dot(yw[...], wide(ehi), preferred_element_type=F32)
            + jnp.dot(yw[...], wide(elo), preferred_element_type=F32))
        for k in range(2):
            sbuf[o, k, 0:dims, :] = value[:, chunks(k)]
            sbuf[o, k, dims:PAD, :] = jnp.broadcast_to(mass[:, chunks(k)], (PAD - dims, LANES))

    V = max(1, G // 4)
    order = [o % G for o in range(1, G + 1)]
    sets = [order[i:i + V] for i in range(0, G, V)]

    def compute(which):
        for o in which:
            source_sums(o)
        for o in which:
            to_partner(o).start()

    def relay(which):
        for o in which:
            to_partner(o).wait_recv()
            pbuf[o] = sbuf[o, core] + prec[o]
            if o:
                to_owner(o).start()

    turns = list(range(1, S)) + [0]
    target_sums(turns[:2])
    finish(copies)
    factor = sig / (cbuf[...] + sum(crec[o] for o in range(S - 1)))
    for b in range(CB):
        row = factor[b:b + 1, :]
        with_mass(yw, chunks(b), y_ref[:, chunks(b)] * row, row)
    rest = turns[2:]
    for k, which in enumerate(sets):
        compute(which)
        if k == 0 and rest:
            target_sums(rest)
        if k == 2 or k == len(sets) - 1 < 2:
            finish([sent_target(o) for o in range(1, S)])
            total = wbuf[0] + sum(wrec[o] for o in range(S - 1))
            tbuf[...] = total[0:dims] / total[dims:dims + 1]
            tcopies = to_column(tbuf, trec, tsend, trecv)
            begin(tcopies)
            to_ref[:, span(me_s, QW)] = tbuf[...]
        relay(which)

    total = pbuf[0]
    for o in range(1, G):
        to_owner(o).wait()
        total = total + srec[o - 1]
    so_ref[...] = total[0:dims] / total[dims:dims + 1]

    def sent(o, _):
        to_partner(o).wait_send()
        return 0

    lax.fori_loop(0, G, sent, 0)
    finish(tcopies)
    for o in range(1, S):
        to_ref[:, span(lax.rem(me_s + S - o, S), QW)] = trec[o - 1]


def delivered(s_ref, t_ref, so_ref, to_ref):
    so_ref[...] = s_ref[...]
    to_ref[...] = t_ref[...]


def shards(S, T, source_pca, target_pca, source_labels, target_labels, block_mask):
    dims, R = source_pca.shape
    C = target_pca.shape[1]
    G = T // 2
    CB, RB = C // LANES, R // LANES
    vmem = pltpu.VMEM
    dma = pltpu.SemaphoreType.DMA
    whole = pl.BlockSpec(memory_space=pltpu.VMEM)
    raw = pl.pallas_call(
        functools.partial(kernel, S, T),
        out_shape=(jax.ShapeDtypeStruct((dims, R // T), F32), jax.ShapeDtypeStruct((dims, C), F32)),
        in_specs=[pl.BlockSpec(memory_space=pl.ANY)] + [whole] * 4,
        out_specs=(whole, whole),
        scratch_shapes=[
            vmem((dims, R), F32), vmem((RB, LANES), F32), dma((R // min(512, R // 2),)),
            vmem((4 * dims, R), BF16), vmem((C, 4 * dims), BF16), vmem((RB, C, LANES), F32),
            vmem((RB, C, LANES), BF16), vmem((RB, C, LANES), BF16), vmem((GROUP, R), F32),
            vmem((C, LANES), F32), vmem((C, LANES), F32), vmem((C, LANES), F32),
            vmem((C, LANES), F32),
            vmem((2 * dims + 2 * GROUP, R), BF16), vmem((2 * dims + 2 * GROUP, C), BF16),
            vmem((2, RB // 2, LANES), F32), vmem((G - 1, RB // 2, LANES), F32),
            vmem((RB // 2, LANES), F32), vmem((RB // 2, LANES), F32), vmem((2, RB // 2, LANES), F32),
            vmem((CB, LANES), F32), vmem((CB, LANES), F32), vmem((S - 1, CB, LANES), F32),
            vmem((2, RB // 2, LANES), F32), vmem((G - 1, RB // 2, LANES), F32),
            vmem((RB // 2, LANES), F32), vmem((RB // 2, LANES), F32), vmem((2, RB // 2, LANES), F32),
            vmem((CB, LANES), F32), vmem((S - 1, CB, LANES), F32),
            vmem((S, PAD, C // S), F32), vmem((S - 1, PAD, C // S), F32),
            vmem((dims, C // S), F32), vmem((S - 1, dims, C // S), F32),
            vmem((G, 2, PAD, LANES), F32), vmem((G, PAD, LANES), F32), vmem((G, PAD, LANES), F32),
            vmem((G - 1, PAD, LANES), F32),
            dma((G - 1,)), dma((G - 1,)), dma((2,)), dma((2,)), dma((S - 1,)), dma((S - 1,)),
            dma((G - 1,)), dma((G - 1,)), dma((2,)), dma((2,)), dma((S - 1,)), dma((S - 1,)),
            dma((S - 1,)), dma((S - 1,)), dma((S - 1,)), dma((S - 1,)),
            dma((G,)), dma((G,)), dma((G - 1,)), dma((G - 1,)),
        ],
        compiler_params=pltpu.CompilerParams(
            collective_id=0, has_side_effects=True, vmem_limit_bytes=60 * 2**20),
    )(source_pca, target_pca, source_labels.reshape(1, R), target_labels.reshape(1, C), block_mask)
    return pl.pallas_call(
        delivered,
        out_shape=tuple(jax.ShapeDtypeStruct(r.shape, F32) for r in raw),
        in_specs=[whole] * 2,
        out_specs=(whole, whole),
    )(*raw)


def solution(mesh):
    placed = (P(None, "src"), P(None, "tgt"), P("src"), P("tgt"), P())
    return jax.shard_map(
        functools.partial(shards, mesh.shape["src"], mesh.shape["tgt"]),
        mesh=mesh,
        in_specs=placed,
        out_specs=(P(None, ("src", "tgt")), P(None, "tgt")),
        check_vma=False,
    )
```

```python
import functools
import math

import jax
import jax.numpy as jnp
from jax import lax
from jax.experimental import pallas as pl
from jax.experimental.pallas import tpu as pltpu
from jax.sharding import PartitionSpec as P

ITERS = 2
EPSILON = 0.05
BARRED = -(2.0**100)
MESH = pl.DeviceIdType.MESH
F32 = jnp.float32
BF16 = jnp.bfloat16
LANES = 128
GROUP = 8
PAD = 72


def in_two(value):
    first = value.astype(BF16)
    return first, (value - first.astype(F32)).astype(BF16)


def turned(row):
    return jnp.broadcast_to(row, (LANES, LANES)).T


def lse_of(parts):
    top = functools.reduce(jnp.maximum, parts)
    return top + jnp.log2(sum(jnp.exp2(p - top) for p in parts))


def span(index, size):
    return pl.ds(pl.multiple_of(index * size, size), size)


def kernel(S, T, x_hbm, y_ref, sl_ref, tl_ref, mask_ref, so_ref, to_ref,
           x_ref, nbuf, fetched, xa, ya, zr, ehi, elo, frow, mp, mb, sp, sb, xw, yw,
           lbuf, lrec, lpair, lown, lprec, mbuf, gbuf, grec,
           rbuf, rrec, rpair, rown, rprec, cbuf, crec,
           wbuf, wrec, tbuf, trec, sbuf, prec, pbuf, srec,
           lsend, lrecv, psend, precv, gsend, grecv,
           rsend, rrecv, qsend, qrecv, csend, crecv,
           wsend, wrecv, tsend, trecv, bsend, brecv, ssend, srecv):
    dims, R = x_ref.shape
    C = y_ref.shape[1]
    G = T // 2
    QW = C // S
    CB = C // LANES
    RB = R // LANES
    scale = math.log2(math.e) / (EPSILON * dims)
    me_s, me_t = lax.axis_index("src"), lax.axis_index("tgt")
    core = lax.rem(me_t, 2)
    chip = me_t // 2
    partner = me_t + 1 - 2 * core

    GZ = min(4, G)
    GX = G // GZ
    offsets = sorted(
        ((dx, dz) for dx in range(GX) for dz in range(GZ)),
        key=lambda d: min(d[0], GX - d[0]) + min(d[1], GZ - d[1]))
    offsets = offsets[:1] + offsets[:0:-1]

    def chip_at(o):
        dx, dz = offsets[o]
        return lax.rem(chip // GZ + dx, GX) * GZ + lax.rem(lax.rem(chip, GZ) + dz, GZ)

    def mate(o):
        return (me_s, 2 * chip_at(o) + core)

    def above(o):
        return (lax.rem(me_s + o, S), me_t)

    pair = (me_s, partner)
    everyone = [mate(o) for o in range(1, G)] + [above(o) for o in range(1, S)] + [pair]
    barrier = pltpu.get_barrier_semaphore()
    for device in everyone:
        pl.semaphore_signal(barrier, inc=1, device_id=device, device_id_type=MESH)

    def remote(src, dst, send, recv, device):
        return pltpu.make_async_remote_copy(
            src_ref=src, dst_ref=dst, send_sem=send, recv_sem=recv,
            device_id=device, device_id_type=MESH)

    def to_mates(src, dst, send, recv):
        return [remote(src, dst.at[o - 1], send, recv, mate(o)) for o in range(1, G)]

    def to_column(src, dst, send, recv):
        return [remote(src, dst.at[o - 1], send, recv, above(o)) for o in range(1, S)]

    def all_of(dst, send, recv):
        return remote(dst, dst, send, recv, pair)

    def begin(copies):
        for copy in copies:
            copy.start()

    def chunks(q):
        return slice(q * LANES, (q + 1) * LANES)

    XC = min(512, R // 2)

    half = R // 2
    half_rows = RB // 2

    def natural(slot):
        return slot + core - 2 * slot * core

    def source_place(c):
        place = natural(c // (half // XC)) * half + lax.rem(c, half // XC) * XC
        return pl.ds(pl.multiple_of(place, XC), XC)

    def fetch(c):
        place = source_place(c)
        return pltpu.make_async_copy(x_hbm.at[:, place], x_ref.at[:, place], fetched.at[c])

    for c in range(R // XC):
        fetch(c).start()

    def prepare_source(c, _):
        at = span(c, XC)
        place = source_place(c)
        fetch(c).wait()
        x = x_ref[:, place]
        x1, x2 = in_two(x)
        for k, part in enumerate((x1, x2, x1)):
            xa[k * dims:(k + 1) * dims, at] = part
        ids = lax.broadcasted_iota(jnp.int32, (dims, XC), 0)
        xa[3 * dims:, at] = jnp.where(ids == sl_ref[:, place], 1.0, 0.0).astype(BF16)
        norm = -scale * jnp.sum(x * x, 0, keepdims=True)
        for k in range(XC // LANES):
            nbuf[pl.ds(c * (XC // LANES) + k, 1), :] = norm[:, chunks(k)]
        return 0

    y = y_ref[...]
    y1, y2 = (p.astype(F32) for p in in_two(2.0 * scale * y))
    ids = lax.broadcasted_iota(jnp.int32, (dims, C), 0)
    onehot = jnp.where(ids == tl_ref[...], 1.0, 0.0).astype(BF16)
    allowed = jnp.dot(mask_ref[...].astype(F32).astype(BF16), onehot, preferred_element_type=F32)
    penalty = jnp.where(allowed > 0.5, 0.0, BARRED)
    for k, (a, b) in enumerate(((y1, y1), (y2, penalty))):
        ya[:, k * LANES:(k + 1) * LANES] = jnp.concatenate([a, b], 0).T.astype(BF16)
    norm = -scale * jnp.sum(y * y, 0, keepdims=True)
    for b in range(CB):
        mb[b * LANES:(b + 1) * LANES, :] = turned(norm[:, chunks(b)])
    lax.fori_loop(0, R // XC, prepare_source, 0)

    block = 2 * LANES
    sub = 16 * GROUP

    def first_rows(slot):
        behind = None
        for u in range(half // block + 1):
            ahead = None
            if u < half // block:
                at = slice(slot * half + u * block, slot * half + (u + 1) * block)
                z = jnp.dot(ya[...], xa[:, at], preferred_element_type=F32)
                ahead = []
                for k in range(2):
                    tops = None
                    for i in range(C // sub):
                        rows = slice(i * sub, (i + 1) * sub)
                        part = z[rows, chunks(k)] + mb[rows, :]
                        zr[slot * half_rows + 2 * u + k, rows, :] = part
                        tops = part if tops is None else jnp.maximum(tops, part)
                    ahead.append(jnp.max(tops, 0, keepdims=True))
            if behind is not None:
                for k in range(2):
                    row, top = 2 * (u - 1) + k, behind[k]
                    total = sum(
                        jnp.exp2(zr[slot * half_rows + row, i * sub:(i + 1) * sub, :] - top)
                        for i in range(C // sub))
                    lbuf[slot, row:row + 1, :] = top + jnp.log2(jnp.sum(total, 0, keepdims=True))
            behind = ahead

    first_rows(1)
    pl.semaphore_wait(barrier, len(everyone))
    early = remote(lbuf.at[1], lprec.at[0], psend.at[0], precv.at[0], pair)
    early.start()
    first_rows(0)
    early.wait()
    lpair[...] = lse_of([lbuf[0], lprec[0]])
    begin(to_mates(lpair, lrec, lsend, lrecv))
    all_of(lrec, lsend, lrecv).wait()
    lown[...] = -math.log2(R * S) - (
        lse_of([lpair[...]] + [lrec[o] for o in range(G - 1)]) + nbuf[0:half_rows, :])
    late = remote(lown, lprec.at[1], psend.at[1], precv.at[1], pair)
    late.start()

    def lanes_of(slot, q):
        return slice(slot * half + q * LANES, slot * half + (q + 1) * LANES)

    def spread(slot, value):
        for q in range(half_rows):
            frow[:, lanes_of(slot, q)] = jnp.broadcast_to(value[q:q + 1, :], (GROUP, LANES))

    WIDE = 4

    def parts_of(value):
        return [value[g * GROUP:(g + 1) * GROUP] for g in range(value.shape[0] // GROUP)]

    def by_rows(slot, step, combine, into, more):

        def body(j, _):
            at = span(j, WIDE * GROUP)
            acc = [[None, None] for _ in range(WIDE)]
            for q in range(half_rows):
                row = frow[:, lanes_of(slot, q)]
                for g, z in enumerate(parts_of(zr[slot * half_rows + q, at, :])):
                    value = step(z, row)
                    old = acc[g][q % 2]
                    acc[g][q % 2] = value if old is None else combine(old, value)
            value = jnp.concatenate([combine(*pair_) for pair_ in acc], 0)
            into[at, :] = combine(into[at, :], value) if more else value
            return 0

        lax.fori_loop(0, C // (WIDE * GROUP), body, 0)

    spread(0, lown[...] + nbuf[0:half_rows, :])
    by_rows(0, jnp.add, jnp.maximum, mp, False)
    late.wait()
    spread(1, lprec[1] + nbuf[half_rows:, :])
    by_rows(1, jnp.add, jnp.maximum, mp, True)

    for b in range(CB):
        rows = slice(b * LANES, (b + 1) * LANES)
        top = jnp.max(mp[rows, :].T, 0, keepdims=True)
        mbuf[b:b + 1, :] = top
        mb[rows, :] = turned(top)

    def weigh(j, _):
        at = span(j, WIDE * GROUP)
        peak = mb[at, :]
        acc = [None, None]
        for q in range(RB):
            row = jnp.concatenate([frow[:, chunks(q)]] * WIDE, 0)
            e = jnp.exp2(zr[q, at, :] + row - peak)
            zr[q, at, :] = e
            acc[q % 2] = e if acc[q % 2] is None else acc[q % 2] + e
        sp[at, :] = acc[0] + acc[1]
        return 0

    lax.fori_loop(0, C // (WIDE * GROUP), weigh, 0)
    for b in range(CB):
        rows = slice(b * LANES, (b + 1) * LANES)
        total = jnp.sum(sp[rows, :].T, 0, keepdims=True)
        gbuf[b:b + 1, :] = mbuf[b:b + 1, :] + jnp.log2(total)

    begin(to_column(gbuf, grec, gsend, grecv))

    def halve(j, _):
        at = span(j, 4 * GROUP)
        for q in range(RB):
            ehi[q, at, :], elo[q, at, :] = in_two(zr[q, at, :])
        return 0

    lax.fori_loop(0, C // (4 * GROUP), halve, 0)
    all_of(grec, gsend, grecv).wait()
    lse = lse_of([gbuf[...]] + [grec[o] for o in range(S - 1)])
    sig = jnp.exp2(mbuf[...] - lse)
    mbuf[...] = sig
    for b in range(CB):
        sb[b * LANES:(b + 1) * LANES, :] = turned(sig[b:b + 1, :])

    def row_mass(slot):

        def body(j, acc):
            at = span(j, WIDE * GROUP)
            acc = list(acc)
            weights = parts_of(sb[at, :])
            for q in range(half_rows):
                terms = [z * w for z, w in zip(parts_of(zr[slot * half_rows + q, at, :]), weights)]
                acc[q] = acc[q] + ((terms[0] + terms[1]) + (terms[2] + terms[3]))
            return tuple(acc)

        zero = jnp.zeros((GROUP, LANES), F32)
        acc = lax.fori_loop(0, C // (WIDE * GROUP), body, (zero,) * half_rows)
        for q, part in enumerate(acc):
            rbuf[slot, q:q + 1, :] = jnp.sum(part, 0, keepdims=True)

    row_mass(1)
    early = remote(rbuf.at[1], rprec.at[0], qsend.at[0], qrecv.at[0], pair)
    early.start()
    row_mass(0)
    early.wait()
    rpair[...] = rbuf[0] + rprec[0]
    begin(to_mates(rpair, rrec, rsend, rrecv))
    all_of(rrec, rsend, rrecv).wait()
    rown[...] = (C * T / (R * S)) / (rpair[...] + sum(rrec[o] for o in range(G - 1)))
    late = remote(rown, rprec.at[1], qsend.at[1], qrecv.at[1], pair)
    late.start()
    spread(0, rown[...])
    by_rows(0, jnp.multiply, jnp.add, sp, False)
    late.wait()
    spread(1, rprec[1])
    by_rows(1, jnp.multiply, jnp.add, sp, True)
    for b in range(CB):
        rows = slice(b * LANES, (b + 1) * LANES)
        cbuf[b:b + 1, :] = sig[b:b + 1, :] * jnp.sum(sp[rows, :].T, 0, keepdims=True)
    begin(to_column(cbuf, crec, csend, crecv))

    tail = lax.broadcasted_iota(jnp.int32, (2 * GROUP, LANES), 0)

    def with_mass(dst, at, value, mass):
        hi, lo = in_two(value)
        dst[0:dims, at] = hi
        dst[dims:2 * dims, at] = lo
        m1, m2 = (p.astype(F32) for p in in_two(mass))
        dst[2 * dims:2 * dims + 2 * GROUP, at] = jnp.where(
            tail == 0, m1, jnp.where(tail == 1, m2, 0.0)).astype(BF16)

    for q in range(RB):
        row = frow[0:1, chunks(q)]
        place = natural(q // half_rows) * half + (q % half_rows) * LANES
        place = pl.ds(pl.multiple_of(place, LANES), LANES)
        with_mass(xw, chunks(q), x_ref[:, place] * row, row)

    def folded(out):
        value = out[0:dims] + out[dims:2 * dims]
        mass = jnp.sum(out[2 * dims:], 0, keepdims=True)
        return value, mass

    across = (((1,), (1,)), ((), ()))

    def sent_target(o):
        return remote(wbuf.at[o], wrec.at[o - 1], wsend, wrecv, above(o))

    def target_sums(*which):
        width = QW if len(which) > 1 else LANES
        pieces = [(o, p) for o in which for p in range(0, QW, width)]
        owner = [lax.rem(me_s + o, S) for o in range(S)]
        outs = [None] * len(pieces)
        depth = min(8, RB)
        for k in range(0, RB, depth):
            left = xw[:, k * LANES:(k + depth) * LANES]
            for ref in (ehi, elo):
                for i, (o, p) in enumerate(pieces):
                    at = pl.ds(pl.multiple_of(owner[o] * QW + p, width), width)
                    right = jnp.concatenate([ref[q, at, :] for q in range(k, k + depth)], 1)
                    part = lax.dot_general(left, right, across, preferred_element_type=F32)
                    outs[i] = part if outs[i] is None else outs[i] + part
        for (o, p), out in zip(pieces, outs):
            value, mass = folded(out)
            for b in range(width // LANES):
                at = slice(p + b * LANES, p + (b + 1) * LANES)
                row = mbuf[pl.ds(owner[o] * (QW // LANES) + p // LANES + b, 1), :]
                wbuf[o, 0:dims, at] = value[:, chunks(b)] * row
                wbuf[o, dims:PAD, at] = jnp.broadcast_to(
                    mass[:, chunks(b)] * row, (PAD - dims, LANES))
        for o in which:
            if o:
                sent_target(o).start()

    V = max(1, G // 4)
    order = [o % G for o in range(1, G + 1)]
    sets = [order[i:i + V] for i in range(0, G, V)]

    def to_partner(k):
        at = pl.ds(k * V, V)
        return remote(sbuf.at[1 - core, at], prec.at[at], bsend.at[k], brecv.at[k], pair)

    def to_owner(o):
        rows = pl.ds(0, dims + 1)
        return remote(pbuf.at[o, rows], srec.at[o - 1, rows], ssend, srecv, mate(o))

    def source_sums(o):
        owner = chip_at(o)
        place = natural(owner // (G // 2)) * half_rows + lax.rem(owner, G // 2) * 2

        def wide(ref):
            return jnp.concatenate([ref[place], ref[place + 1]], 1)

        value, mass = folded(
            jnp.dot(yw[...], wide(ehi), preferred_element_type=F32)
            + jnp.dot(yw[...], wide(elo), preferred_element_type=F32))
        for k in range(2):
            sbuf[k, (o - 1) % G, 0:dims, :] = value[:, chunks(k)]
            sbuf[k, (o - 1) % G, dims:PAD, :] = jnp.broadcast_to(
                mass[:, chunks(k)], (PAD - dims, LANES))

    def compute(k):
        for o in sets[k]:
            source_sums(o)
        to_partner(k).start()

    def relay(k):
        to_partner(k).wait_recv()
        for o in sets[k]:
            pbuf[o] = sbuf[core, (o - 1) % G] + prec[(o - 1) % G]
        for o in sets[k]:
            if o:
                to_owner(o).start()

    for o in range(1, S, 2):
        target_sums(*range(o, min(o + 2, S)))
    all_of(crec, csend, crecv).wait()
    factor = sig / (cbuf[...] + sum(crec[o] for o in range(S - 1)))
    for b in range(CB):
        row = factor[b:b + 1, :]
        with_mass(yw, chunks(b), y_ref[:, chunks(b)] * row, row)
    compute(0)
    compute(1)
    relay(0)
    target_sums(0)
    relay(1)
    if len(sets) > 2:
        compute(2)
    all_of(wrec, wsend, wrecv).wait()
    total = wbuf[0] + sum(wrec[o] for o in range(S - 1))
    tbuf[...] = total[0:dims] / total[dims:dims + 1]
    begin(to_column(tbuf, trec, tsend, trecv))
    to_ref[:, span(me_s, QW)] = tbuf[...]
    for k in range(2, len(sets)):
        relay(k)
        if k + 1 < len(sets):
            compute(k + 1)

    arrived = srec.at[:, pl.ds(0, dims + 1)]
    remote(arrived, arrived, ssend, srecv, pair).wait()
    total = pbuf[0, 0:dims] + sum(srec[o, 0:dims] for o in range(G - 1))
    mass = pbuf[0, dims:dims + 1] + sum(srec[o, dims:dims + 1] for o in range(G - 1))
    so_ref[...] = total / mass

    for k in range(len(sets)):
        to_partner(k).wait_send()
    all_of(trec, tsend, trecv).wait()
    for o in range(1, S):
        to_ref[:, span(lax.rem(me_s + S - o, S), QW)] = trec[o - 1]


def delivered(s_ref, t_ref, so_hbm, to_hbm, sems):
    copies = [pltpu.make_async_copy(src, dst, sems.at[k])
              for k, (src, dst) in enumerate(((t_ref, to_hbm), (s_ref, so_hbm)))]
    for copy in copies:
        copy.start()
    for copy in copies:
        copy.wait()


def shards(S, T, source_pca, target_pca, source_labels, target_labels, block_mask):
    dims, R = source_pca.shape
    C = target_pca.shape[1]
    G = T // 2
    CB, RB = C // LANES, R // LANES
    sets = min(4, G)
    vmem = pltpu.VMEM
    dma = pltpu.SemaphoreType.DMA
    whole = pl.BlockSpec(memory_space=pltpu.VMEM)
    raw = pl.pallas_call(
        functools.partial(kernel, S, T),
        out_shape=(vmem((dims, R // T), F32), vmem((dims, C), F32)),
        in_specs=[pl.BlockSpec(memory_space=pl.ANY)] + [whole] * 4,
        out_specs=(whole, whole),
        scratch_shapes=[
            vmem((dims, R), F32), vmem((RB, LANES), F32), dma((R // min(512, R // 2),)),
            vmem((4 * dims, R), BF16), vmem((C, 4 * dims), BF16), vmem((RB, C, LANES), F32),
            vmem((RB, C, LANES), BF16), vmem((RB, C, LANES), BF16), vmem((GROUP, R), F32),
            vmem((C, LANES), F32), vmem((C, LANES), F32), vmem((C, LANES), F32),
            vmem((C, LANES), F32),
            vmem((2 * dims + 2 * GROUP, R), BF16), vmem((2 * dims + 2 * GROUP, C), BF16),
            vmem((2, RB // 2, LANES), F32), vmem((G - 1, RB // 2, LANES), F32),
            vmem((RB // 2, LANES), F32), vmem((RB // 2, LANES), F32), vmem((2, RB // 2, LANES), F32),
            vmem((CB, LANES), F32), vmem((CB, LANES), F32), vmem((S - 1, CB, LANES), F32),
            vmem((2, RB // 2, LANES), F32), vmem((G - 1, RB // 2, LANES), F32),
            vmem((RB // 2, LANES), F32), vmem((RB // 2, LANES), F32), vmem((2, RB // 2, LANES), F32),
            vmem((CB, LANES), F32), vmem((S - 1, CB, LANES), F32),
            vmem((S, PAD, C // S), F32), vmem((S - 1, PAD, C // S), F32),
            vmem((dims, C // S), F32), vmem((S - 1, dims, C // S), F32),
            vmem((2, G, PAD, LANES), F32), vmem((G, PAD, LANES), F32), vmem((G, PAD, LANES), F32),
            vmem((G - 1, PAD, LANES), F32),
            dma, dma, dma((2,)), dma((2,)), dma, dma,
            dma, dma, dma((2,)), dma((2,)), dma, dma,
            dma, dma, dma, dma, dma((sets,)), dma((sets,)), dma, dma,
        ],
        compiler_params=pltpu.CompilerParams(
            collective_id=0, has_side_effects=True, vmem_limit_bytes=56 * 2**20),
    )(source_pca, target_pca, source_labels.reshape(1, R), target_labels.reshape(1, C), block_mask)
    return pl.pallas_call(
        delivered,
        out_shape=tuple(jax.ShapeDtypeStruct(r.shape, F32) for r in raw),
        in_specs=[whole] * 2,
        out_specs=(pl.BlockSpec(memory_space=pl.ANY),) * 2,
        scratch_shapes=[dma((2,))],
    )(*(pltpu.with_memory_space_constraint(r, pltpu.VMEM) for r in raw))


def solution(mesh):
    placed = (P(None, "src"), P(None, "tgt"), P("src"), P("tgt"), P())
    return jax.shard_map(
        functools.partial(shards, mesh.shape["src"], mesh.shape["tgt"]),
        mesh=mesh,
        in_specs=placed,
        out_specs=(P(None, ("src", "tgt")), P(None, "tgt")),
        check_vma=False,
    )
```

```python
import functools
import math

import jax
import jax.numpy as jnp
from jax import lax
from jax.experimental import pallas as pl
from jax.experimental.pallas import tpu as pltpu
from jax.sharding import PartitionSpec as P

ITERS = 2
EPSILON = 0.05
BARRED = -(2.0**100)
MESH = pl.DeviceIdType.MESH
F32 = jnp.float32
BF16 = jnp.bfloat16
LANES = 128
GROUP = 8
PAD = 72


def in_two(value):
    first = value.astype(BF16)
    return first, (value - first.astype(F32)).astype(BF16)


def turned(row):
    return jnp.broadcast_to(row, (LANES, LANES)).T


def lse_of(parts):
    top = functools.reduce(jnp.maximum, parts)
    return top + jnp.log2(sum(jnp.exp2(p - top) for p in parts))


def span(index, size):
    return pl.ds(pl.multiple_of(index * size, size), size)


def kernel(S, T, x_hbm, y_ref, sl_ref, tl_ref, mask_ref, so_ref, to_ref,
           x_ref, nbuf, fetched, xa, ya, zr, ehi, elo, frow, mp, mb, sp, sb, xw, yw,
           lbuf, lrec, lpair, lown, lprec, mbuf, gbuf, grec,
           rbuf, rrec, rpair, rown, rprec, cbuf, crec,
           wbuf, wrec, tbuf, trec, sbuf, prec, pbuf, srec,
           lsend, lrecv, psend, precv, gsend, grecv,
           rsend, rrecv, qsend, qrecv, csend, crecv,
           wsend, wrecv, tsend, trecv, bsend, brecv, ssend, srecv):
    dims, R = x_ref.shape
    C = y_ref.shape[1]
    G = T // 2
    QW = C // S
    CB = C // LANES
    RB = R // LANES
    scale = math.log2(math.e) / (EPSILON * dims)
    me_s, me_t = lax.axis_index("src"), lax.axis_index("tgt")
    core = lax.rem(me_t, 2)
    chip = me_t // 2
    partner = me_t + 1 - 2 * core

    GZ = min(4, G)
    GX = G // GZ
    offsets = sorted(
        ((dx, dz) for dx in range(GX) for dz in range(GZ)),
        key=lambda d: min(d[0], GX - d[0]) + min(d[1], GZ - d[1]))
    offsets = offsets[:1] + offsets[:0:-1]

    def chip_at(o):
        dx, dz = offsets[o]
        return lax.rem(chip // GZ + dx, GX) * GZ + lax.rem(lax.rem(chip, GZ) + dz, GZ)

    def mate(o):
        return (me_s, 2 * chip_at(o) + core)

    def above(o):
        return (lax.rem(me_s + o, S), me_t)

    pair = (me_s, partner)
    everyone = [mate(o) for o in range(1, G)] + [above(o) for o in range(1, S)] + [pair]
    barrier = pltpu.get_barrier_semaphore()
    for device in everyone:
        pl.semaphore_signal(barrier, inc=1, device_id=device, device_id_type=MESH)

    def remote(src, dst, send, recv, device):
        return pltpu.make_async_remote_copy(
            src_ref=src, dst_ref=dst, send_sem=send, recv_sem=recv,
            device_id=device, device_id_type=MESH)

    def to_mates(src, dst, send, recv):
        return [remote(src, dst.at[o - 1], send, recv, mate(o)) for o in range(1, G)]

    def to_column(src, dst, send, recv):
        return [remote(src, dst.at[o - 1], send, recv, above(o)) for o in range(1, S)]

    def all_of(dst, send, recv):
        return remote(dst, dst, send, recv, pair)

    def begin(copies):
        for copy in copies:
            copy.start()

    def chunks(q):
        return slice(q * LANES, (q + 1) * LANES)

    XC = min(512, R // 2)

    half = R // 2
    half_rows = RB // 2

    def natural(slot):
        return slot + core - 2 * slot * core

    def source_place(c):
        place = natural(c // (half // XC)) * half + lax.rem(c, half // XC) * XC
        return pl.ds(pl.multiple_of(place, XC), XC)

    def fetch(c):
        place = source_place(c)
        return pltpu.make_async_copy(x_hbm.at[:, place], x_ref.at[:, place], fetched.at[c])

    for c in range(R // XC):
        fetch(c).start()

    def prepare_source(c, _):
        at = span(c, XC)
        place = source_place(c)
        fetch(c).wait()
        x = x_ref[:, place]
        x1, x2 = in_two(x)
        for k, part in enumerate((x1, x2, x1)):
            xa[k * dims:(k + 1) * dims, at] = part
        ids = lax.broadcasted_iota(jnp.int32, (dims, XC), 0)
        xa[3 * dims:, at] = jnp.where(ids == sl_ref[:, place], 1.0, 0.0).astype(BF16)
        norm = -scale * jnp.sum(x * x, 0, keepdims=True)
        for k in range(XC // LANES):
            nbuf[pl.ds(c * (XC // LANES) + k, 1), :] = norm[:, chunks(k)]
        return 0

    y = y_ref[...]
    y1, y2 = (p.astype(F32) for p in in_two(2.0 * scale * y))
    ids = lax.broadcasted_iota(jnp.int32, (dims, C), 0)
    onehot = jnp.where(ids == tl_ref[...], 1.0, 0.0).astype(BF16)
    allowed = jnp.dot(mask_ref[...].astype(F32).astype(BF16), onehot, preferred_element_type=F32)
    penalty = jnp.where(allowed > 0.5, 0.0, BARRED)
    for k, (a, b) in enumerate(((y1, y1), (y2, penalty))):
        ya[:, k * LANES:(k + 1) * LANES] = jnp.concatenate([a, b], 0).T.astype(BF16)
    norm = -scale * jnp.sum(y * y, 0, keepdims=True)
    for b in range(CB):
        mb[b * LANES:(b + 1) * LANES, :] = turned(norm[:, chunks(b)])
    lax.fori_loop(0, R // XC, prepare_source, 0)

    block = 2 * LANES
    sub = 16 * GROUP

    def first_rows(slot):
        behind = None
        for u in range(half // block + 1):
            ahead = None
            if u < half // block:
                at = slice(slot * half + u * block, slot * half + (u + 1) * block)
                z = jnp.dot(ya[...], xa[:, at], preferred_element_type=F32)
                ahead = []
                for k in range(2):
                    tops = None
                    for i in range(C // sub):
                        rows = slice(i * sub, (i + 1) * sub)
                        part = z[rows, chunks(k)] + mb[rows, :]
                        zr[slot * half_rows + 2 * u + k, rows, :] = part
                        tops = part if tops is None else jnp.maximum(tops, part)
                    ahead.append(jnp.max(tops, 0, keepdims=True))
            if behind is not None:
                for k in range(2):
                    row, top = 2 * (u - 1) + k, behind[k]
                    total = sum(
                        jnp.exp2(zr[slot * half_rows + row, i * sub:(i + 1) * sub, :] - top)
                        for i in range(C // sub))
                    lbuf[slot, row:row + 1, :] = top + jnp.log2(jnp.sum(total, 0, keepdims=True))
            behind = ahead

    first_rows(1)
    pl.semaphore_wait(barrier, len(everyone))
    early = remote(lbuf.at[1], lprec.at[0], psend.at[0], precv.at[0], pair)
    early.start()
    first_rows(0)
    early.wait()
    lpair[...] = lse_of([lbuf[0], lprec[0]])
    begin(to_mates(lpair, lrec, lsend, lrecv))
    all_of(lrec, lsend, lrecv).wait()
    lown[...] = -math.log2(R * S) - (
        lse_of([lpair[...]] + [lrec[o] for o in range(G - 1)]) + nbuf[0:half_rows, :])
    late = remote(lown, lprec.at[1], psend.at[1], precv.at[1], pair)
    late.start()

    def lanes_of(slot, q):
        return slice(slot * half + q * LANES, slot * half + (q + 1) * LANES)

    def spread(slot, value):
        for q in range(half_rows):
            frow[:, lanes_of(slot, q)] = jnp.broadcast_to(value[q:q + 1, :], (GROUP, LANES))

    WIDE = 4

    def parts_of(value):
        return [value[g * GROUP:(g + 1) * GROUP] for g in range(value.shape[0] // GROUP)]

    def by_rows(slot, step, combine, into, more):

        def body(j, _):
            at = span(j, WIDE * GROUP)
            acc = [[None, None] for _ in range(WIDE)]
            for q in range(half_rows):
                row = frow[:, lanes_of(slot, q)]
                for g, z in enumerate(parts_of(zr[slot * half_rows + q, at, :])):
                    value = step(z, row)
                    old = acc[g][q % 2]
                    acc[g][q % 2] = value if old is None else combine(old, value)
            value = jnp.concatenate([combine(*pair_) for pair_ in acc], 0)
            into[at, :] = combine(into[at, :], value) if more else value
            return 0

        lax.fori_loop(0, C // (WIDE * GROUP), body, 0)

    spread(0, lown[...] + nbuf[0:half_rows, :])
    by_rows(0, jnp.add, jnp.maximum, mp, False)
    late.wait()
    spread(1, lprec[1] + nbuf[half_rows:, :])
    by_rows(1, jnp.add, jnp.maximum, mp, True)

    for b in range(CB):
        rows = slice(b * LANES, (b + 1) * LANES)
        top = jnp.max(mp[rows, :].T, 0, keepdims=True)
        mbuf[b:b + 1, :] = top
        mb[rows, :] = turned(top)

    def weigh(j, _):
        at = span(j, WIDE * GROUP)
        peak = mb[at, :]
        acc = [None, None]
        for q in range(RB):
            row = jnp.concatenate([frow[:, chunks(q)]] * WIDE, 0)
            e = jnp.exp2(zr[q, at, :] + row - peak)
            zr[q, at, :] = e
            acc[q % 2] = e if acc[q % 2] is None else acc[q % 2] + e
        sp[at, :] = acc[0] + acc[1]
        return 0

    lax.fori_loop(0, C // (WIDE * GROUP), weigh, 0)
    for b in range(CB):
        rows = slice(b * LANES, (b + 1) * LANES)
        total = jnp.sum(sp[rows, :].T, 0, keepdims=True)
        gbuf[b:b + 1, :] = mbuf[b:b + 1, :] + jnp.log2(total)

    begin(to_column(gbuf, grec, gsend, grecv))

    def halve(j, _):
        at = span(j, 4 * GROUP)
        for q in range(RB):
            ehi[q, at, :], elo[q, at, :] = in_two(zr[q, at, :])
        return 0

    lax.fori_loop(0, C // (4 * GROUP), halve, 0)
    all_of(grec, gsend, grecv).wait()
    lse = lse_of([gbuf[...]] + [grec[o] for o in range(S - 1)])
    sig = jnp.exp2(mbuf[...] - lse)
    mbuf[...] = sig
    for b in range(CB):
        sb[b * LANES:(b + 1) * LANES, :] = turned(sig[b:b + 1, :])

    def row_mass(slot):

        def body(j, acc):
            at = span(j, WIDE * GROUP)
            acc = list(acc)
            weights = parts_of(sb[at, :])
            for q in range(half_rows):
                terms = [z * w for z, w in zip(parts_of(zr[slot * half_rows + q, at, :]), weights)]
                acc[q] = acc[q] + ((terms[0] + terms[1]) + (terms[2] + terms[3]))
            return tuple(acc)

        zero = jnp.zeros((GROUP, LANES), F32)
        acc = lax.fori_loop(0, C // (WIDE * GROUP), body, (zero,) * half_rows)
        for q, part in enumerate(acc):
            rbuf[slot, q:q + 1, :] = jnp.sum(part, 0, keepdims=True)

    row_mass(1)
    early = remote(rbuf.at[1], rprec.at[0], qsend.at[0], qrecv.at[0], pair)
    early.start()
    row_mass(0)
    early.wait()
    rpair[...] = rbuf[0] + rprec[0]
    begin(to_mates(rpair, rrec, rsend, rrecv))
    all_of(rrec, rsend, rrecv).wait()
    rown[...] = (C * T / (R * S)) / (rpair[...] + sum(rrec[o] for o in range(G - 1)))
    late = remote(rown, rprec.at[1], qsend.at[1], qrecv.at[1], pair)
    late.start()
    tail = lax.broadcasted_iota(jnp.int32, (2 * GROUP, LANES), 0)

    def with_mass(dst, at, value, mass):
        hi, lo = in_two(value)
        dst[0:dims, at] = hi
        dst[dims:2 * dims, at] = lo
        m1, m2 = (p.astype(F32) for p in in_two(mass))
        dst[2 * dims:2 * dims + 2 * GROUP, at] = jnp.where(
            tail == 0, m1, jnp.where(tail == 1, m2, 0.0)).astype(BF16)

    def scale_source(slot):
        for q in range(slot * half_rows, (slot + 1) * half_rows):
            row = frow[0:1, chunks(q)]
            place = natural(slot) * half + (q % half_rows) * LANES
            place = pl.ds(pl.multiple_of(place, LANES), LANES)
            with_mass(xw, chunks(q), x_ref[:, place] * row, row)

    spread(0, rown[...])
    by_rows(0, jnp.multiply, jnp.add, sp, False)
    scale_source(0)
    late.wait()
    spread(1, rprec[1])
    by_rows(1, jnp.multiply, jnp.add, sp, True)
    for b in range(CB):
        rows = slice(b * LANES, (b + 1) * LANES)
        cbuf[b:b + 1, :] = sig[b:b + 1, :] * jnp.sum(sp[rows, :].T, 0, keepdims=True)
    begin(to_column(cbuf, crec, csend, crecv))

    scale_source(1)

    def folded(out):
        value = out[0:dims] + out[dims:2 * dims]
        mass = jnp.sum(out[2 * dims:], 0, keepdims=True)
        return value, mass

    across = (((1,), (1,)), ((), ()))

    def sent_target(o):
        return remote(wbuf.at[o], wrec.at[o - 1], wsend, wrecv, above(o))

    def target_sums(*which):
        width = QW if len(which) > 1 else LANES
        pieces = [(o, p) for o in which for p in range(0, QW, width)]
        owner = [lax.rem(me_s + o, S) for o in range(S)]
        outs = [None] * len(pieces)
        depth = min(8, RB)
        for k in range(0, RB, depth):
            left = xw[:, k * LANES:(k + depth) * LANES]
            for ref in (ehi, elo):
                for i, (o, p) in enumerate(pieces):
                    at = pl.ds(pl.multiple_of(owner[o] * QW + p, width), width)
                    right = jnp.concatenate([ref[q, at, :] for q in range(k, k + depth)], 1)
                    part = lax.dot_general(left, right, across, preferred_element_type=F32)
                    outs[i] = part if outs[i] is None else outs[i] + part
        for (o, p), out in zip(pieces, outs):
            value, mass = folded(out)
            for b in range(width // LANES):
                at = slice(p + b * LANES, p + (b + 1) * LANES)
                row = mbuf[pl.ds(owner[o] * (QW // LANES) + p // LANES + b, 1), :]
                wbuf[o, 0:dims, at] = value[:, chunks(b)] * row
                wbuf[o, dims:PAD, at] = jnp.broadcast_to(
                    mass[:, chunks(b)] * row, (PAD - dims, LANES))
        for o in which:
            if o:
                sent_target(o).start()

    V = max(1, G // 4)
    order = [o % G for o in range(1, G + 1)]
    sets = [order[i:i + V] for i in range(0, G, V)]

    def to_partner(k):
        at = pl.ds(k * V, V)
        return remote(sbuf.at[1 - core, at], prec.at[at], bsend.at[k], brecv.at[k], pair)

    def to_owner(o):
        rows = pl.ds(0, dims + 1)
        return remote(pbuf.at[o, rows], srec.at[o - 1, rows], ssend, srecv, mate(o))

    def source_sums(o):
        owner = chip_at(o)
        place = natural(owner // (G // 2)) * half_rows + lax.rem(owner, G // 2) * 2

        def wide(ref):
            return jnp.concatenate([ref[place], ref[place + 1]], 1)

        value, mass = folded(
            jnp.dot(yw[...], wide(ehi), preferred_element_type=F32)
            + jnp.dot(yw[...], wide(elo), preferred_element_type=F32))
        for k in range(2):
            sbuf[k, (o - 1) % G, 0:dims, :] = value[:, chunks(k)]
            sbuf[k, (o - 1) % G, dims:PAD, :] = jnp.broadcast_to(
                mass[:, chunks(k)], (PAD - dims, LANES))

    def compute(k):
        for o in sets[k]:
            source_sums(o)
        to_partner(k).start()

    def relay(k):
        to_partner(k).wait_recv()
        for o in sets[k]:
            pbuf[o] = sbuf[core, (o - 1) % G] + prec[(o - 1) % G]
        for o in sets[k]:
            if o:
                to_owner(o).start()

    target_sums(*range(1, min(3, S)))
    all_of(crec, csend, crecv).wait()
    factor = sig / (cbuf[...] + sum(crec[o] for o in range(S - 1)))
    for b in range(CB):
        row = factor[b:b + 1, :]
        with_mass(yw, chunks(b), y_ref[:, chunks(b)] * row, row)
    compute(0)
    compute(1)
    relay(0)
    if S > 3:
        target_sums(*range(3, S))
    relay(1)
    for k in range(2, len(sets)):
        compute(k)
    for k in range(2, len(sets) - 1):
        relay(k)
    target_sums(0)
    if len(sets) > 2:
        relay(len(sets) - 1)
    all_of(wrec, wsend, wrecv).wait()
    total = wbuf[0] + sum(wrec[o] for o in range(S - 1))
    tbuf[...] = total[0:dims] / total[dims:dims + 1]
    begin(to_column(tbuf, trec, tsend, trecv))
    to_ref[:, span(me_s, QW)] = tbuf[...]

    arrived = srec.at[:, pl.ds(0, dims + 1)]
    remote(arrived, arrived, ssend, srecv, pair).wait()
    total = pbuf[0, 0:dims] + sum(srec[o, 0:dims] for o in range(G - 1))
    mass = pbuf[0, dims:dims + 1] + sum(srec[o, dims:dims + 1] for o in range(G - 1))
    so_ref[...] = total / mass

    for k in range(len(sets)):
        to_partner(k).wait_send()
    all_of(trec, tsend, trecv).wait()
    for o in range(1, S):
        to_ref[:, span(lax.rem(me_s + S - o, S), QW)] = trec[o - 1]


def delivered(s_ref, t_ref, so_hbm, to_hbm, sems):
    copies = [pltpu.make_async_copy(src, dst, sems.at[k])
              for k, (src, dst) in enumerate(((t_ref, to_hbm), (s_ref, so_hbm)))]
    for copy in copies:
        copy.start()
    for copy in copies:
        copy.wait()


def shards(S, T, source_pca, target_pca, source_labels, target_labels, block_mask):
    dims, R = source_pca.shape
    C = target_pca.shape[1]
    G = T // 2
    CB, RB = C // LANES, R // LANES
    sets = min(4, G)
    vmem = pltpu.VMEM
    dma = pltpu.SemaphoreType.DMA
    whole = pl.BlockSpec(memory_space=pltpu.VMEM)
    raw = pl.pallas_call(
        functools.partial(kernel, S, T),
        out_shape=(vmem((dims, R // T), F32), vmem((dims, C), F32)),
        in_specs=[pl.BlockSpec(memory_space=pl.ANY)] + [whole] * 4,
        out_specs=(whole, whole),
        scratch_shapes=[
            vmem((dims, R), F32), vmem((RB, LANES), F32), dma((R // min(512, R // 2),)),
            vmem((4 * dims, R), BF16), vmem((C, 4 * dims), BF16), vmem((RB, C, LANES), F32),
            vmem((RB, C, LANES), BF16), vmem((RB, C, LANES), BF16), vmem((GROUP, R), F32),
            vmem((C, LANES), F32), vmem((C, LANES), F32), vmem((C, LANES), F32),
            vmem((C, LANES), F32),
            vmem((2 * dims + 2 * GROUP, R), BF16), vmem((2 * dims + 2 * GROUP, C), BF16),
            vmem((2, RB // 2, LANES), F32), vmem((G - 1, RB // 2, LANES), F32),
            vmem((RB // 2, LANES), F32), vmem((RB // 2, LANES), F32), vmem((2, RB // 2, LANES), F32),
            vmem((CB, LANES), F32), vmem((CB, LANES), F32), vmem((S - 1, CB, LANES), F32),
            vmem((2, RB // 2, LANES), F32), vmem((G - 1, RB // 2, LANES), F32),
            vmem((RB // 2, LANES), F32), vmem((RB // 2, LANES), F32), vmem((2, RB // 2, LANES), F32),
            vmem((CB, LANES), F32), vmem((S - 1, CB, LANES), F32),
            vmem((S, PAD, C // S), F32), vmem((S - 1, PAD, C // S), F32),
            vmem((dims, C // S), F32), vmem((S - 1, dims, C // S), F32),
            vmem((2, G, PAD, LANES), F32), vmem((G, PAD, LANES), F32), vmem((G, PAD, LANES), F32),
            vmem((G - 1, PAD, LANES), F32),
            dma, dma, dma((2,)), dma((2,)), dma, dma,
            dma, dma, dma((2,)), dma((2,)), dma, dma,
            dma, dma, dma, dma, dma((sets,)), dma((sets,)), dma, dma,
        ],
        compiler_params=pltpu.CompilerParams(
            collective_id=0, has_side_effects=True, vmem_limit_bytes=56 * 2**20),
    )(source_pca, target_pca, source_labels.reshape(1, R), target_labels.reshape(1, C), block_mask)
    return pl.pallas_call(
        delivered,
        out_shape=tuple(jax.ShapeDtypeStruct(r.shape, F32) for r in raw),
        in_specs=[whole] * 2,
        out_specs=(pl.BlockSpec(memory_space=pl.ANY),) * 2,
        scratch_shapes=[dma((2,))],
    )(*(pltpu.with_memory_space_constraint(r, pltpu.VMEM) for r in raw))


def solution(mesh):
    placed = (P(None, "src"), P(None, "tgt"), P("src"), P("tgt"), P())
    return jax.shard_map(
        functools.partial(shards, mesh.shape["src"], mesh.shape["tgt"]),
        mesh=mesh,
        in_specs=placed,
        out_specs=(P(None, ("src", "tgt")), P(None, "tgt")),
        check_vma=False,
    )
```

```python
import functools
import math

import jax
import jax.numpy as jnp
from jax import lax
from jax.experimental import pallas as pl
from jax.experimental.pallas import tpu as pltpu
from jax.sharding import PartitionSpec as P

ITERS = 2
EPSILON = 0.05
BARRED = -(2.0**100)
MESH = pl.DeviceIdType.MESH
F32 = jnp.float32
BF16 = jnp.bfloat16
LANES = 128
GROUP = 8
PAD = 72


def in_two(value):
    first = value.astype(BF16)
    return first, (value - first.astype(F32)).astype(BF16)


def turned(row):
    return jnp.broadcast_to(row, (LANES, LANES)).T


def lse_of(parts):
    top = functools.reduce(jnp.maximum, parts)
    return top + jnp.log2(sum(jnp.exp2(p - top) for p in parts))


def span(index, size):
    return pl.ds(pl.multiple_of(index * size, size), size)


def kernel(S, T, x_hbm, y_ref, sl_ref, tl_ref, mask_ref, so_ref, to_ref,
           x_ref, nbuf, ylow, fetched, xa, ya, zr, ehi, elo, frow, mp, mb, sp, sb, xw, yw,
           lbuf, lrec, lpair, lown, lprec, mbuf, gbuf, grec,
           rbuf, rrec, rpair, rown, rprec, cbuf, crec,
           wbuf, wrec, tbuf, trec, sbuf, prec, pbuf, srec,
           lsend, lrecv, psend, precv, gsend, grecv,
           rsend, rrecv, qsend, qrecv, csend, crecv,
           wsend, wrecv, tsend, trecv, bsend, brecv, ssend, srecv):
    dims, R = x_ref.shape
    C = y_ref.shape[1]
    G = T // 2
    QW = C // S
    CB = C // LANES
    RB = R // LANES
    scale = math.log2(math.e) / (EPSILON * dims)
    me_s, me_t = lax.axis_index("src"), lax.axis_index("tgt")
    core = lax.rem(me_t, 2)
    chip = me_t // 2
    partner = me_t + 1 - 2 * core

    GZ = min(4, G)
    GX = G // GZ
    offsets = sorted(
        ((dx, dz) for dx in range(GX) for dz in range(GZ)),
        key=lambda d: min(d[0], GX - d[0]) + min(d[1], GZ - d[1]))
    offsets = offsets[:1] + offsets[:0:-1]

    def chip_at(o):
        dx, dz = offsets[o]
        return lax.rem(chip // GZ + dx, GX) * GZ + lax.rem(lax.rem(chip, GZ) + dz, GZ)

    def mate(o):
        return (me_s, 2 * chip_at(o) + core)

    def above(o):
        return (lax.rem(me_s + o, S), me_t)

    pair = (me_s, partner)
    everyone = [mate(o) for o in range(1, G)] + [above(o) for o in range(1, S)] + [pair]
    barrier = pltpu.get_barrier_semaphore()
    for device in everyone:
        pl.semaphore_signal(barrier, inc=1, device_id=device, device_id_type=MESH)

    def remote(src, dst, send, recv, device):
        return pltpu.make_async_remote_copy(
            src_ref=src, dst_ref=dst, send_sem=send, recv_sem=recv,
            device_id=device, device_id_type=MESH)

    def to_mates(src, dst, send, recv):
        return [remote(src, dst.at[o - 1], send, recv, mate(o)) for o in range(1, G)]

    def to_column(src, dst, send, recv):
        return [remote(src, dst.at[o - 1], send, recv, above(o)) for o in range(1, S)]

    def all_of(dst, send, recv):
        return remote(dst, dst, send, recv, pair)

    def begin(copies):
        for copy in copies:
            copy.start()

    def chunks(q):
        return slice(q * LANES, (q + 1) * LANES)

    XC = min(512, R // 2)

    half = R // 2
    half_rows = RB // 2

    def natural(slot):
        return slot + core - 2 * slot * core

    def source_place(c):
        place = natural(c // (half // XC)) * half + lax.rem(c, half // XC) * XC
        return pl.ds(pl.multiple_of(place, XC), XC)

    def fetch(c):
        place = source_place(c)
        return pltpu.make_async_copy(x_hbm.at[:, place], x_ref.at[:, place], fetched.at[c])

    for c in range(R // XC):
        fetch(c).start()

    def prepare_source(c, _):
        at = span(c, XC)
        place = source_place(c)
        fetch(c).wait()
        x = x_ref[:, place]
        x1, x2 = in_two(x)
        for k, part in enumerate((x1, x2, x1)):
            xa[k * dims:(k + 1) * dims, at] = part
        ids = lax.broadcasted_iota(jnp.int32, (dims, XC), 0)
        xa[3 * dims:, at] = jnp.where(ids == sl_ref[:, place], 1.0, 0.0).astype(BF16)
        norm = -scale * jnp.sum(x * x, 0, keepdims=True)
        for k in range(XC // LANES):
            nbuf[pl.ds(c * (XC // LANES) + k, 1), :] = norm[:, chunks(k)]
        return 0

    y = y_ref[...]
    y1, y2 = (p.astype(F32) for p in in_two(2.0 * scale * y))
    ids = lax.broadcasted_iota(jnp.int32, (dims, C), 0)
    onehot = jnp.where(ids == tl_ref[...], 1.0, 0.0).astype(BF16)
    allowed = jnp.dot(mask_ref[...].astype(F32).astype(BF16), onehot, preferred_element_type=F32)
    norm = -scale * jnp.sum(y * y, 0, keepdims=True)
    rounded = norm.astype(BF16).astype(F32)
    penalty = jnp.where(allowed > 0.5, rounded, BARRED)
    for k, (a, b) in enumerate(((y1, y1), (y2, penalty))):
        ya[:, k * LANES:(k + 1) * LANES] = jnp.concatenate([a, b], 0).T.astype(BF16)
    remainder = norm - rounded
    for b in range(CB):
        ylow[b:b + 1, :] = remainder[:, chunks(b)]
        mb[b * LANES:(b + 1) * LANES, :] = turned(jnp.exp2(remainder[:, chunks(b)]))
    lax.fori_loop(0, R // XC, prepare_source, 0)

    block = min(2 * LANES, half)
    sub = 4 * GROUP

    def first_rows(slot):
        behind = None
        wide = block // LANES
        for u in range(half // block + 1):
            ahead = None
            if u < half // block:
                at = slice(slot * half + u * block, slot * half + (u + 1) * block)
                z = jnp.dot(ya[...], xa[:, at], preferred_element_type=F32)
                ahead = []
                for k in range(wide):
                    zr[slot * half_rows + wide * u + k] = z[:, chunks(k)]
                    tops = functools.reduce(
                        jnp.maximum, [z[i:i + sub, chunks(k)] for i in range(0, C, sub)])
                    ahead.append(jnp.max(tops, 0, keepdims=True))
            if behind is not None:
                totals = [None] * wide
                for i in range(0, C, sub):
                    weight = mb[i:i + sub, :]
                    for k in range(wide):
                        row = slot * half_rows + wide * (u - 1) + k
                        e = jnp.exp2(zr[row, i:i + sub, :] - behind[k]) * weight
                        totals[k] = e if totals[k] is None else totals[k] + e
                for k in range(wide):
                    row = wide * (u - 1) + k
                    lbuf[slot, row:row + 1, :] = behind[k] + jnp.log2(
                        jnp.sum(totals[k], 0, keepdims=True))
            behind = ahead

    first_rows(1)
    pl.semaphore_wait(barrier, len(everyone))
    early = remote(lbuf.at[1], lprec.at[0], psend.at[0], precv.at[0], pair)
    early.start()
    first_rows(0)
    early.wait()
    lpair[...] = lse_of([lbuf[0], lprec[0]])
    begin(to_mates(lpair, lrec, lsend, lrecv))
    all_of(lrec, lsend, lrecv).wait()
    lown[...] = -math.log2(R * S) - (
        lse_of([lpair[...]] + [lrec[o] for o in range(G - 1)]) + nbuf[0:half_rows, :])
    late = remote(lown, lprec.at[1], psend.at[1], precv.at[1], pair)
    late.start()

    def lanes_of(slot, q):
        return slice(slot * half + q * LANES, slot * half + (q + 1) * LANES)

    def spread(slot, value):
        for q in range(half_rows):
            frow[:, lanes_of(slot, q)] = jnp.broadcast_to(value[q:q + 1, :], (GROUP, LANES))

    WIDE = 4

    def parts_of(value):
        return [value[g * GROUP:(g + 1) * GROUP] for g in range(value.shape[0] // GROUP)]

    def by_rows(slot, step, combine, into, more):

        def body(j, _):
            at = span(j, WIDE * GROUP)
            acc = [[None, None] for _ in range(WIDE)]
            for q in range(half_rows):
                row = frow[:, lanes_of(slot, q)]
                for g, z in enumerate(parts_of(zr[slot * half_rows + q, at, :])):
                    value = step(z, row)
                    old = acc[g][q % 2]
                    acc[g][q % 2] = value if old is None else combine(old, value)
            value = jnp.concatenate([combine(*pair_) for pair_ in acc], 0)
            into[at, :] = combine(into[at, :], value) if more else value
            return 0

        lax.fori_loop(0, C // (WIDE * GROUP), body, 0)

    spread(0, lown[...] + nbuf[0:half_rows, :])
    by_rows(0, jnp.add, jnp.maximum, mp, False)
    late.wait()
    spread(1, lprec[1] + nbuf[half_rows:, :])
    by_rows(1, jnp.add, jnp.maximum, mp, True)

    for b in range(CB):
        rows = slice(b * LANES, (b + 1) * LANES)
        top = jnp.max(mp[rows, :].T, 0, keepdims=True)
        mbuf[b:b + 1, :] = top
        mb[rows, :] = turned(top)

    def weigh(j, _):
        at = span(j, WIDE * GROUP)
        peak = mb[at, :]
        acc = [None, None]
        for q in range(RB):
            row = jnp.concatenate([frow[:, chunks(q)]] * WIDE, 0)
            e = jnp.exp2(zr[q, at, :] + row - peak)
            zr[q, at, :] = e
            acc[q % 2] = e if acc[q % 2] is None else acc[q % 2] + e
        sp[at, :] = acc[0] + acc[1]
        return 0

    lax.fori_loop(0, C // (WIDE * GROUP), weigh, 0)
    for b in range(CB):
        rows = slice(b * LANES, (b + 1) * LANES)
        total = jnp.sum(sp[rows, :].T, 0, keepdims=True)
        gbuf[b:b + 1, :] = mbuf[b:b + 1, :] + ylow[b:b + 1, :] + jnp.log2(total)

    begin(to_column(gbuf, grec, gsend, grecv))

    def halve(j, _):
        at = span(j, 4 * GROUP)
        for q in range(RB):
            ehi[q, at, :], elo[q, at, :] = in_two(zr[q, at, :])
        return 0

    lax.fori_loop(0, C // (4 * GROUP), halve, 0)
    all_of(grec, gsend, grecv).wait()
    lse = lse_of([gbuf[...]] + [grec[o] for o in range(S - 1)])
    sig = jnp.exp2(mbuf[...] + ylow[...] - lse)
    mbuf[...] = sig
    for b in range(CB):
        sb[b * LANES:(b + 1) * LANES, :] = turned(sig[b:b + 1, :])

    def row_mass(slot):

        def body(j, acc):
            at = span(j, WIDE * GROUP)
            acc = list(acc)
            weights = parts_of(sb[at, :])
            for q in range(half_rows):
                terms = [z * w for z, w in zip(parts_of(zr[slot * half_rows + q, at, :]), weights)]
                acc[q] = acc[q] + ((terms[0] + terms[1]) + (terms[2] + terms[3]))
            return tuple(acc)

        zero = jnp.zeros((GROUP, LANES), F32)
        acc = lax.fori_loop(0, C // (WIDE * GROUP), body, (zero,) * half_rows)
        for q, part in enumerate(acc):
            rbuf[slot, q:q + 1, :] = jnp.sum(part, 0, keepdims=True)

    row_mass(1)
    early = remote(rbuf.at[1], rprec.at[0], qsend.at[0], qrecv.at[0], pair)
    early.start()
    row_mass(0)
    early.wait()
    rpair[...] = rbuf[0] + rprec[0]
    begin(to_mates(rpair, rrec, rsend, rrecv))
    all_of(rrec, rsend, rrecv).wait()
    rown[...] = (C * T / (R * S)) / (rpair[...] + sum(rrec[o] for o in range(G - 1)))
    late = remote(rown, rprec.at[1], qsend.at[1], qrecv.at[1], pair)
    late.start()
    tail = lax.broadcasted_iota(jnp.int32, (2 * GROUP, LANES), 0)

    def with_mass(dst, at, value, mass):
        hi, lo = in_two(value)
        dst[0:dims, at] = hi
        dst[dims:2 * dims, at] = lo
        m1, m2 = (p.astype(F32) for p in in_two(mass))
        dst[2 * dims:2 * dims + 2 * GROUP, at] = jnp.where(
            tail == 0, m1, jnp.where(tail == 1, m2, 0.0)).astype(BF16)

    def scale_source(slot):
        for q in range(slot * half_rows, (slot + 1) * half_rows):
            row = frow[0:1, chunks(q)]
            place = natural(slot) * half + (q % half_rows) * LANES
            place = pl.ds(pl.multiple_of(place, LANES), LANES)
            with_mass(xw, chunks(q), x_ref[:, place] * row, row)

    spread(0, rown[...])
    by_rows(0, jnp.multiply, jnp.add, sp, False)
    scale_source(0)
    late.wait()
    spread(1, rprec[1])
    by_rows(1, jnp.multiply, jnp.add, sp, True)
    for b in range(CB):
        rows = slice(b * LANES, (b + 1) * LANES)
        cbuf[b:b + 1, :] = sig[b:b + 1, :] * jnp.sum(sp[rows, :].T, 0, keepdims=True)
    begin(to_column(cbuf, crec, csend, crecv))

    scale_source(1)

    def folded(out):
        value = out[0:dims] + out[dims:2 * dims]
        mass = jnp.sum(out[2 * dims:], 0, keepdims=True)
        return value, mass

    across = (((1,), (1,)), ((), ()))

    def sent_target(o):
        return remote(wbuf.at[o], wrec.at[o - 1], wsend, wrecv, above(o))

    def target_sums(*which):
        width = QW if len(which) > 1 else LANES
        pieces = [(o, p) for o in which for p in range(0, QW, width)]
        owner = [lax.rem(me_s + o, S) for o in range(S)]
        outs = [None] * len(pieces)
        depth = min(8, RB)
        for k in range(0, RB, depth):
            left = xw[:, k * LANES:(k + depth) * LANES]
            for ref in (ehi, elo):
                for i, (o, p) in enumerate(pieces):
                    at = pl.ds(pl.multiple_of(owner[o] * QW + p, width), width)
                    right = jnp.concatenate([ref[q, at, :] for q in range(k, k + depth)], 1)
                    part = lax.dot_general(left, right, across, preferred_element_type=F32)
                    outs[i] = part if outs[i] is None else outs[i] + part
        for (o, p), out in zip(pieces, outs):
            value, mass = folded(out)
            for b in range(width // LANES):
                at = slice(p + b * LANES, p + (b + 1) * LANES)
                row = mbuf[pl.ds(owner[o] * (QW // LANES) + p // LANES + b, 1), :]
                wbuf[o, 0:dims, at] = value[:, chunks(b)] * row
                wbuf[o, dims:PAD, at] = jnp.broadcast_to(
                    mass[:, chunks(b)] * row, (PAD - dims, LANES))
        for o in which:
            if o:
                sent_target(o).start()

    V = max(1, G // 4)
    order = [o % G for o in range(1, G + 1)]
    sets = [order[i:i + V] for i in range(0, G, V)]

    def to_partner(k):
        at = pl.ds(k * V, V)
        return remote(sbuf.at[1 - core, at], prec.at[at], bsend.at[k], brecv.at[k], pair)

    def to_owner(o):
        rows = pl.ds(0, dims + 1)
        return remote(pbuf.at[o, rows], srec.at[o - 1, rows], ssend, srecv, mate(o))

    def source_sums(o):
        owner = chip_at(o)
        place = natural(owner // (G // 2)) * half_rows + lax.rem(owner, G // 2) * 2

        def wide(ref):
            return jnp.concatenate([ref[place], ref[place + 1]], 1)

        value, mass = folded(
            jnp.dot(yw[...], wide(ehi), preferred_element_type=F32)
            + jnp.dot(yw[...], wide(elo), preferred_element_type=F32))
        for k in range(2):
            sbuf[k, (o - 1) % G, 0:dims, :] = value[:, chunks(k)]
            sbuf[k, (o - 1) % G, dims:PAD, :] = jnp.broadcast_to(
                mass[:, chunks(k)], (PAD - dims, LANES))

    def compute(k):
        for o in sets[k]:
            source_sums(o)
        to_partner(k).start()

    def relay(k):
        to_partner(k).wait_recv()
        for o in sets[k]:
            pbuf[o] = sbuf[core, (o - 1) % G] + prec[(o - 1) % G]
        for o in sets[k]:
            if o:
                to_owner(o).start()

    target_sums(*range(1, min(3, S)))
    all_of(crec, csend, crecv).wait()
    factor = sig / (cbuf[...] + sum(crec[o] for o in range(S - 1)))
    for b in range(CB):
        row = factor[b:b + 1, :]
        with_mass(yw, chunks(b), y_ref[:, chunks(b)] * row, row)
    compute(0)
    compute(1)
    relay(0)
    if S > 3:
        target_sums(*range(3, S))
    relay(1)
    for k in range(2, len(sets)):
        compute(k)
    for k in range(2, len(sets) - 1):
        relay(k)
    target_sums(0)
    if len(sets) > 2:
        relay(len(sets) - 1)
    all_of(wrec, wsend, wrecv).wait()
    total = wbuf[0] + sum(wrec[o] for o in range(S - 1))
    tbuf[...] = total[0:dims] / total[dims:dims + 1]
    begin(to_column(tbuf, trec, tsend, trecv))
    to_ref[:, span(me_s, QW)] = tbuf[...]

    arrived = srec.at[:, pl.ds(0, dims + 1)]
    remote(arrived, arrived, ssend, srecv, pair).wait()
    total = pbuf[0, 0:dims] + sum(srec[o, 0:dims] for o in range(G - 1))
    mass = pbuf[0, dims:dims + 1] + sum(srec[o, dims:dims + 1] for o in range(G - 1))
    so_ref[...] = total / mass

    for k in range(len(sets)):
        to_partner(k).wait_send()
    all_of(trec, tsend, trecv).wait()
    for o in range(1, S):
        to_ref[:, span(lax.rem(me_s + S - o, S), QW)] = trec[o - 1]


def delivered(s_ref, t_ref, so_hbm, to_hbm, sems):
    copies = [pltpu.make_async_copy(src, dst, sems.at[k])
              for k, (src, dst) in enumerate(((t_ref, to_hbm), (s_ref, so_hbm)))]
    for copy in copies:
        copy.start()
    for copy in copies:
        copy.wait()


def shards(S, T, source_pca, target_pca, source_labels, target_labels, block_mask):
    dims, R = source_pca.shape
    C = target_pca.shape[1]
    G = T // 2
    CB, RB = C // LANES, R // LANES
    sets = min(4, G)
    vmem = pltpu.VMEM
    dma = pltpu.SemaphoreType.DMA
    whole = pl.BlockSpec(memory_space=pltpu.VMEM)
    raw = pl.pallas_call(
        functools.partial(kernel, S, T),
        out_shape=(vmem((dims, R // T), F32), vmem((dims, C), F32)),
        in_specs=[pl.BlockSpec(memory_space=pl.ANY)] + [whole] * 4,
        out_specs=(whole, whole),
        scratch_shapes=[
            vmem((dims, R), F32), vmem((RB, LANES), F32), vmem((CB, LANES), F32), dma((R // min(512, R // 2),)),
            vmem((4 * dims, R), BF16), vmem((C, 4 * dims), BF16), vmem((RB, C, LANES), F32),
            vmem((RB, C, LANES), BF16), vmem((RB, C, LANES), BF16), vmem((GROUP, R), F32),
            vmem((C, LANES), F32), vmem((C, LANES), F32), vmem((C, LANES), F32),
            vmem((C, LANES), F32),
            vmem((2 * dims + 2 * GROUP, R), BF16), vmem((2 * dims + 2 * GROUP, C), BF16),
            vmem((2, RB // 2, LANES), F32), vmem((G - 1, RB // 2, LANES), F32),
            vmem((RB // 2, LANES), F32), vmem((RB // 2, LANES), F32), vmem((2, RB // 2, LANES), F32),
            vmem((CB, LANES), F32), vmem((CB, LANES), F32), vmem((S - 1, CB, LANES), F32),
            vmem((2, RB // 2, LANES), F32), vmem((G - 1, RB // 2, LANES), F32),
            vmem((RB // 2, LANES), F32), vmem((RB // 2, LANES), F32), vmem((2, RB // 2, LANES), F32),
            vmem((CB, LANES), F32), vmem((S - 1, CB, LANES), F32),
            vmem((S, PAD, C // S), F32), vmem((S - 1, PAD, C // S), F32),
            vmem((dims, C // S), F32), vmem((S - 1, dims, C // S), F32),
            vmem((2, G, PAD, LANES), F32), vmem((G, PAD, LANES), F32), vmem((G, PAD, LANES), F32),
            vmem((G - 1, PAD, LANES), F32),
            dma, dma, dma((2,)), dma((2,)), dma, dma,
            dma, dma, dma((2,)), dma((2,)), dma, dma,
            dma, dma, dma, dma, dma((sets,)), dma((sets,)), dma, dma,
        ],
        compiler_params=pltpu.CompilerParams(
            collective_id=0, has_side_effects=True, vmem_limit_bytes=56 * 2**20),
    )(source_pca, target_pca, source_labels.reshape(1, R), target_labels.reshape(1, C), block_mask)
    return pl.pallas_call(
        delivered,
        out_shape=tuple(jax.ShapeDtypeStruct(r.shape, F32) for r in raw),
        in_specs=[whole] * 2,
        out_specs=(pl.BlockSpec(memory_space=pl.ANY),) * 2,
        scratch_shapes=[dma((2,))],
    )(*(pltpu.with_memory_space_constraint(r, pltpu.VMEM) for r in raw))


def solution(mesh):
    placed = (P(None, "src"), P(None, "tgt"), P("src"), P("tgt"), P())
    return jax.shard_map(
        functools.partial(shards, mesh.shape["src"], mesh.shape["tgt"]),
        mesh=mesh,
        in_specs=placed,
        out_specs=(P(None, ("src", "tgt")), P(None, "tgt")),
        check_vma=False,
    )
```

```python
import functools
import math

import jax
import jax.numpy as jnp
from jax import lax
from jax.experimental import pallas as pl
from jax.experimental.pallas import tpu as pltpu
from jax.sharding import PartitionSpec as P

ITERS = 2
EPSILON = 0.05
BARRED = -(2.0**100)
MESH = pl.DeviceIdType.MESH
F32 = jnp.float32
BF16 = jnp.bfloat16
LANES = 128
GROUP = 8
PAD = 72


def in_two(value):
    first = value.astype(BF16)
    return first, (value - first.astype(F32)).astype(BF16)


def turned(row):
    return jnp.broadcast_to(row, (LANES, LANES)).T


def lse_of(parts):
    top = functools.reduce(jnp.maximum, parts)
    return top + jnp.log2(sum(jnp.exp2(p - top) for p in parts))


def span(index, size):
    return pl.ds(pl.multiple_of(index * size, size), size)


def kernel(S, T, x_hbm, y_ref, sl_ref, tl_ref, mask_ref, so_ref, to_ref,
           x_ref, nbuf, fetched, xa, ya, zr, ehi, elo, frow, mp, mb, sp, sb, xw, yw,
           lbuf, lrec, lpair, lown, lprec, mbuf, gbuf, grec,
           rbuf, rrec, rpair, rown, rprec, cbuf, crec,
           wbuf, wrec, tbuf, trec, sbuf, prec, pbuf, srec,
           lsend, lrecv, psend, precv, gsend, grecv,
           rsend, rrecv, qsend, qrecv, csend, crecv,
           wsend, wrecv, tsend, trecv, bsend, brecv, ssend, srecv):
    dims, R = x_ref.shape
    C = y_ref.shape[1]
    G = T // 2
    QW = C // S
    CB = C // LANES
    RB = R // LANES
    scale = math.log2(math.e) / (EPSILON * dims)
    me_s, me_t = lax.axis_index("src"), lax.axis_index("tgt")
    core = lax.rem(me_t, 2)
    chip = me_t // 2
    partner = me_t + 1 - 2 * core

    GZ = min(4, G)
    GX = G // GZ
    offsets = sorted(
        ((dx, dz) for dx in range(GX) for dz in range(GZ)),
        key=lambda d: min(d[0], GX - d[0]) + min(d[1], GZ - d[1]))
    offsets = offsets[:1] + offsets[:0:-1]

    def chip_at(o):
        dx, dz = offsets[o]
        return lax.rem(chip // GZ + dx, GX) * GZ + lax.rem(lax.rem(chip, GZ) + dz, GZ)

    def mate(o):
        return (me_s, 2 * chip_at(o) + core)

    def above(o):
        return (lax.rem(me_s + o, S), me_t)

    pair = (me_s, partner)
    everyone = [mate(o) for o in range(1, G)] + [above(o) for o in range(1, S)] + [pair]
    barrier = pltpu.get_barrier_semaphore()
    for device in everyone:
        pl.semaphore_signal(barrier, inc=1, device_id=device, device_id_type=MESH)

    def remote(src, dst, send, recv, device):
        return pltpu.make_async_remote_copy(
            src_ref=src, dst_ref=dst, send_sem=send, recv_sem=recv,
            device_id=device, device_id_type=MESH)

    def to_mates(src, dst, send, recv):
        return [remote(src, dst.at[o - 1], send, recv, mate(o)) for o in range(1, G)]

    def to_column(src, dst, send, recv):
        return [remote(src, dst.at[o - 1], send, recv, above(o)) for o in range(1, S)]

    def all_of(dst, send, recv):
        return remote(dst, dst, send, recv, pair)

    def begin(copies):
        for copy in copies:
            copy.start()

    def chunks(q):
        return slice(q * LANES, (q + 1) * LANES)

    XC = min(512, R // 2)

    half = R // 2
    half_rows = RB // 2

    def natural(slot):
        return slot + core - 2 * slot * core

    def source_place(c):
        place = natural(c // (half // XC)) * half + lax.rem(c, half // XC) * XC
        return pl.ds(pl.multiple_of(place, XC), XC)

    def fetch(c):
        place = source_place(c)
        return pltpu.make_async_copy(x_hbm.at[:, place], x_ref.at[:, place], fetched.at[c])

    for c in range(R // XC):
        fetch(c).start()

    def prepare_source(c, _):
        at = span(c, XC)
        place = source_place(c)
        fetch(c).wait()
        x = x_ref[:, place]
        x1, x2 = in_two(x)
        for k, part in enumerate((x1, x2, x1)):
            xa[k * dims:(k + 1) * dims, at] = part
        ids = lax.broadcasted_iota(jnp.int32, (dims, XC), 0)
        xa[3 * dims:, at] = jnp.where(ids == sl_ref[:, place], 1.0, 0.0).astype(BF16)
        norm = -scale * jnp.sum(x * x, 0, keepdims=True)
        for k in range(XC // LANES):
            nbuf[pl.ds(c * (XC // LANES) + k, 1), :] = norm[:, chunks(k)]
        return 0

    y = y_ref[...]
    y1, y2 = (p.astype(F32) for p in in_two(2.0 * scale * y))
    ids = lax.broadcasted_iota(jnp.int32, (dims, C), 0)
    onehot = jnp.where(ids == tl_ref[...], 1.0, 0.0).astype(BF16)
    allowed = jnp.dot(mask_ref[...].astype(F32).astype(BF16), onehot, preferred_element_type=F32)
    penalty = jnp.where(allowed > 0.5, 0.0, BARRED)
    for k, (a, b) in enumerate(((y1, y1), (y2, penalty))):
        ya[:, k * LANES:(k + 1) * LANES] = jnp.concatenate([a, b], 0).T.astype(BF16)
    norm = -scale * jnp.sum(y * y, 0, keepdims=True)
    for b in range(CB):
        mb[b * LANES:(b + 1) * LANES, :] = turned(norm[:, chunks(b)])
    lax.fori_loop(0, R // XC, prepare_source, 0)

    block = 2 * LANES
    sub = 16 * GROUP

    def first_rows(slot):
        behind = None
        for u in range(half // block + 1):
            ahead = None
            if u < half // block:
                at = slice(slot * half + u * block, slot * half + (u + 1) * block)
                z = jnp.dot(ya[...], xa[:, at], preferred_element_type=F32)
                ahead = []
                for k in range(2):
                    tops = None
                    for i in range(C // sub):
                        rows = slice(i * sub, (i + 1) * sub)
                        part = z[rows, chunks(k)] + mb[rows, :]
                        zr[slot * half_rows + 2 * u + k, rows, :] = part
                        tops = part if tops is None else jnp.maximum(tops, part)
                    ahead.append(jnp.max(tops, 0, keepdims=True))
            if behind is not None:
                for k in range(2):
                    row, top = 2 * (u - 1) + k, behind[k]
                    total = sum(
                        jnp.exp2(zr[slot * half_rows + row, i * sub:(i + 1) * sub, :] - top)
                        for i in range(C // sub))
                    lbuf[slot, row:row + 1, :] = top + jnp.log2(jnp.sum(total, 0, keepdims=True))
            behind = ahead

    first_rows(1)
    pl.semaphore_wait(barrier, len(everyone))
    early = remote(lbuf.at[1], lprec.at[0], psend.at[0], precv.at[0], pair)
    early.start()
    first_rows(0)
    early.wait()
    lpair[...] = lse_of([lbuf[0], lprec[0]])
    begin(to_mates(lpair, lrec, lsend, lrecv))
    all_of(lrec, lsend, lrecv).wait()
    lown[...] = -math.log2(R * S) - (
        lse_of([lpair[...]] + [lrec[o] for o in range(G - 1)]) + nbuf[0:half_rows, :])
    late = remote(lown, lprec.at[1], psend.at[1], precv.at[1], pair)
    late.start()

    def lanes_of(slot, q):
        return slice(slot * half + q * LANES, slot * half + (q + 1) * LANES)

    def spread(slot, value):
        for q in range(half_rows):
            frow[:, lanes_of(slot, q)] = jnp.broadcast_to(value[q:q + 1, :], (GROUP, LANES))

    WIDE = 8

    def parts_of(value):
        return [value[g * GROUP:(g + 1) * GROUP] for g in range(value.shape[0] // GROUP)]

    def by_rows(slot, step, combine, into, more):

        def body(j, _):
            at = span(j, WIDE * GROUP)
            acc = [[None, None] for _ in range(WIDE)]
            for q in range(half_rows):
                row = frow[:, lanes_of(slot, q)]
                for g, z in enumerate(parts_of(zr[slot * half_rows + q, at, :])):
                    value = step(z, row)
                    old = acc[g][q % 2]
                    acc[g][q % 2] = value if old is None else combine(old, value)
            value = jnp.concatenate([combine(*pair_) for pair_ in acc], 0)
            into[at, :] = combine(into[at, :], value) if more else value
            return 0

        lax.fori_loop(0, C // (WIDE * GROUP), body, 0)

    spread(0, lown[...] + nbuf[0:half_rows, :])
    by_rows(0, jnp.add, jnp.maximum, mp, False)
    late.wait()
    spread(1, lprec[1] + nbuf[half_rows:, :])
    by_rows(1, jnp.add, jnp.maximum, mp, True)

    for b in range(CB):
        rows = slice(b * LANES, (b + 1) * LANES)
        top = jnp.max(mp[rows, :].T, 0, keepdims=True)
        mbuf[b:b + 1, :] = top
        mb[rows, :] = turned(top)

    def weigh(j, _):
        at = span(j, WIDE * GROUP)
        peak = mb[at, :]
        acc = [None, None]
        for q in range(RB):
            row = jnp.concatenate([frow[:, chunks(q)]] * WIDE, 0)
            e = jnp.exp2(zr[q, at, :] + row - peak)
            zr[q, at, :] = e
            acc[q % 2] = e if acc[q % 2] is None else acc[q % 2] + e
        sp[at, :] = acc[0] + acc[1]
        return 0

    lax.fori_loop(0, C // (WIDE * GROUP), weigh, 0)
    for b in range(CB):
        rows = slice(b * LANES, (b + 1) * LANES)
        total = jnp.sum(sp[rows, :].T, 0, keepdims=True)
        gbuf[b:b + 1, :] = mbuf[b:b + 1, :] + jnp.log2(total)

    begin(to_column(gbuf, grec, gsend, grecv))

    def halve(j, _):
        at = span(j, 4 * GROUP)
        for q in range(RB):
            ehi[q, at, :], elo[q, at, :] = in_two(zr[q, at, :])
        return 0

    lax.fori_loop(0, C // (4 * GROUP), halve, 0)
    all_of(grec, gsend, grecv).wait()
    lse = lse_of([gbuf[...]] + [grec[o] for o in range(S - 1)])
    sig = jnp.exp2(mbuf[...] - lse)
    mbuf[...] = sig
    for b in range(CB):
        sb[b * LANES:(b + 1) * LANES, :] = turned(sig[b:b + 1, :])

    def row_mass(slot):

        def body(j, acc):
            at = span(j, WIDE * GROUP)
            acc = list(acc)
            weights = parts_of(sb[at, :])
            for q in range(half_rows):
                terms = [z * w for z, w in zip(parts_of(zr[slot * half_rows + q, at, :]), weights)]
                while len(terms) > 1:
                    terms = [u + v for u, v in zip(terms[::2], terms[1::2])]
                acc[q] = acc[q] + terms[0]
            return tuple(acc)

        zero = jnp.zeros((GROUP, LANES), F32)
        acc = lax.fori_loop(0, C // (WIDE * GROUP), body, (zero,) * half_rows)
        for q, part in enumerate(acc):
            rbuf[slot, q:q + 1, :] = jnp.sum(part, 0, keepdims=True)

    row_mass(1)
    early = remote(rbuf.at[1], rprec.at[0], qsend.at[0], qrecv.at[0], pair)
    early.start()
    row_mass(0)
    early.wait()
    rpair[...] = rbuf[0] + rprec[0]
    begin(to_mates(rpair, rrec, rsend, rrecv))
    all_of(rrec, rsend, rrecv).wait()
    rown[...] = (C * T / (R * S)) / (rpair[...] + sum(rrec[o] for o in range(G - 1)))
    late = remote(rown, rprec.at[1], qsend.at[1], qrecv.at[1], pair)
    late.start()
    tail = lax.broadcasted_iota(jnp.int32, (2 * GROUP, LANES), 0)

    def with_mass(dst, at, value, mass):
        hi, lo = in_two(value)
        dst[0:dims, at] = hi
        dst[dims:2 * dims, at] = lo
        m1, m2 = (p.astype(F32) for p in in_two(mass))
        dst[2 * dims:2 * dims + 2 * GROUP, at] = jnp.where(
            tail == 0, m1, jnp.where(tail == 1, m2, 0.0)).astype(BF16)

    def scale_source(slot):
        for q in range(slot * half_rows, (slot + 1) * half_rows):
            row = frow[0:1, chunks(q)]
            place = natural(slot) * half + (q % half_rows) * LANES
            place = pl.ds(pl.multiple_of(place, LANES), LANES)
            with_mass(xw, chunks(q), x_ref[:, place] * row, row)

    spread(0, rown[...])
    by_rows(0, jnp.multiply, jnp.add, sp, False)
    scale_source(0)
    late.wait()
    spread(1, rprec[1])
    by_rows(1, jnp.multiply, jnp.add, sp, True)
    for b in range(CB):
        rows = slice(b * LANES, (b + 1) * LANES)
        cbuf[b:b + 1, :] = sig[b:b + 1, :] * jnp.sum(sp[rows, :].T, 0, keepdims=True)
    begin(to_column(cbuf, crec, csend, crecv))

    scale_source(1)

    def folded(out):
        value = out[0:dims] + out[dims:2 * dims]
        mass = jnp.sum(out[2 * dims:], 0, keepdims=True)
        return value, mass

    across = (((1,), (1,)), ((), ()))

    def sent_target(o):
        return remote(wbuf.at[o], wrec.at[o - 1], wsend, wrecv, above(o))

    def target_sums(*which):
        width = QW if len(which) > 1 else LANES
        pieces = [(o, p) for o in which for p in range(0, QW, width)]
        owner = [lax.rem(me_s + o, S) for o in range(S)]
        outs = [None] * len(pieces)
        depth = min(8, RB)
        for k in range(0, RB, depth):
            left = xw[:, k * LANES:(k + depth) * LANES]
            for ref in (ehi, elo):
                for i, (o, p) in enumerate(pieces):
                    at = pl.ds(pl.multiple_of(owner[o] * QW + p, width), width)
                    right = jnp.concatenate([ref[q, at, :] for q in range(k, k + depth)], 1)
                    part = lax.dot_general(left, right, across, preferred_element_type=F32)
                    outs[i] = part if outs[i] is None else outs[i] + part
        for (o, p), out in zip(pieces, outs):
            value, mass = folded(out)
            for b in range(width // LANES):
                at = slice(p + b * LANES, p + (b + 1) * LANES)
                row = mbuf[pl.ds(owner[o] * (QW // LANES) + p // LANES + b, 1), :]
                wbuf[o, 0:dims, at] = value[:, chunks(b)] * row
                wbuf[o, dims:PAD, at] = jnp.broadcast_to(
                    mass[:, chunks(b)] * row, (PAD - dims, LANES))
        for o in which:
            if o:
                sent_target(o).start()

    V = max(1, G // 4)
    order = [o % G for o in range(1, G + 1)]
    sets = [order[i:i + V] for i in range(0, G, V)]

    def to_partner(k):
        at = pl.ds(k * V, V)
        return remote(sbuf.at[1 - core, at], prec.at[at], bsend.at[k], brecv.at[k], pair)

    def to_owner(o):
        rows = pl.ds(0, dims + 1)
        return remote(pbuf.at[o, rows], srec.at[o - 1, rows], ssend, srecv, mate(o))

    def source_sums(o):
        owner = chip_at(o)
        place = natural(owner // (G // 2)) * half_rows + lax.rem(owner, G // 2) * 2

        def wide(ref):
            return jnp.concatenate([ref[place], ref[place + 1]], 1)

        value, mass = folded(
            jnp.dot(yw[...], wide(ehi), preferred_element_type=F32)
            + jnp.dot(yw[...], wide(elo), preferred_element_type=F32))
        for k in range(2):
            sbuf[k, (o - 1) % G, 0:dims, :] = value[:, chunks(k)]
            sbuf[k, (o - 1) % G, dims:PAD, :] = jnp.broadcast_to(
                mass[:, chunks(k)], (PAD - dims, LANES))

    def compute(k):
        for o in sets[k]:
            source_sums(o)
        to_partner(k).start()

    def relay(k):
        to_partner(k).wait_recv()
        for o in sets[k]:
            pbuf[o] = sbuf[core, (o - 1) % G] + prec[(o - 1) % G]
        for o in sets[k]:
            if o:
                to_owner(o).start()

    target_sums(*range(1, min(3, S)))
    all_of(crec, csend, crecv).wait()
    factor = sig / (cbuf[...] + sum(crec[o] for o in range(S - 1)))
    for b in range(CB):
        row = factor[b:b + 1, :]
        with_mass(yw, chunks(b), y_ref[:, chunks(b)] * row, row)
    compute(0)
    compute(1)
    relay(0)
    if S > 3:
        target_sums(*range(3, S))
    relay(1)
    for k in range(2, len(sets)):
        compute(k)
    for k in range(2, len(sets) - 1):
        relay(k)
    target_sums(0)
    if len(sets) > 2:
        relay(len(sets) - 1)
    all_of(wrec, wsend, wrecv).wait()
    total = wbuf[0] + sum(wrec[o] for o in range(S - 1))
    tbuf[...] = total[0:dims] / total[dims:dims + 1]
    begin(to_column(tbuf, trec, tsend, trecv))
    to_ref[:, span(me_s, QW)] = tbuf[...]

    arrived = srec.at[:, pl.ds(0, dims + 1)]
    remote(arrived, arrived, ssend, srecv, pair).wait()
    total = pbuf[0, 0:dims] + sum(srec[o, 0:dims] for o in range(G - 1))
    mass = pbuf[0, dims:dims + 1] + sum(srec[o, dims:dims + 1] for o in range(G - 1))
    so_ref[...] = total / mass

    for k in range(len(sets)):
        to_partner(k).wait_send()
    all_of(trec, tsend, trecv).wait()
    for o in range(1, S):
        to_ref[:, span(lax.rem(me_s + S - o, S), QW)] = trec[o - 1]


def delivered(s_ref, t_ref, so_hbm, to_hbm, sems):
    copies = [pltpu.make_async_copy(src, dst, sems.at[k])
              for k, (src, dst) in enumerate(((t_ref, to_hbm), (s_ref, so_hbm)))]
    for copy in copies:
        copy.start()
    for copy in copies:
        copy.wait()


def shards(S, T, source_pca, target_pca, source_labels, target_labels, block_mask):
    dims, R = source_pca.shape
    C = target_pca.shape[1]
    G = T // 2
    CB, RB = C // LANES, R // LANES
    sets = min(4, G)
    vmem = pltpu.VMEM
    dma = pltpu.SemaphoreType.DMA
    whole = pl.BlockSpec(memory_space=pltpu.VMEM)
    raw = pl.pallas_call(
        functools.partial(kernel, S, T),
        out_shape=(vmem((dims, R // T), F32), vmem((dims, C), F32)),
        in_specs=[pl.BlockSpec(memory_space=pl.ANY)] + [whole] * 4,
        out_specs=(whole, whole),
        scratch_shapes=[
            vmem((dims, R), F32), vmem((RB, LANES), F32), dma((R // min(512, R // 2),)),
            vmem((4 * dims, R), BF16), vmem((C, 4 * dims), BF16), vmem((RB, C, LANES), F32),
            vmem((RB, C, LANES), BF16), vmem((RB, C, LANES), BF16), vmem((GROUP, R), F32),
            vmem((C, LANES), F32), vmem((C, LANES), F32), vmem((C, LANES), F32),
            vmem((C, LANES), F32),
            vmem((2 * dims + 2 * GROUP, R), BF16), vmem((2 * dims + 2 * GROUP, C), BF16),
            vmem((2, RB // 2, LANES), F32), vmem((G - 1, RB // 2, LANES), F32),
            vmem((RB // 2, LANES), F32), vmem((RB // 2, LANES), F32), vmem((2, RB // 2, LANES), F32),
            vmem((CB, LANES), F32), vmem((CB, LANES), F32), vmem((S - 1, CB, LANES), F32),
            vmem((2, RB // 2, LANES), F32), vmem((G - 1, RB // 2, LANES), F32),
            vmem((RB // 2, LANES), F32), vmem((RB // 2, LANES), F32), vmem((2, RB // 2, LANES), F32),
            vmem((CB, LANES), F32), vmem((S - 1, CB, LANES), F32),
            vmem((S, PAD, C // S), F32), vmem((S - 1, PAD, C // S), F32),
            vmem((dims, C // S), F32), vmem((S - 1, dims, C // S), F32),
            vmem((2, G, PAD, LANES), F32), vmem((G, PAD, LANES), F32), vmem((G, PAD, LANES), F32),
            vmem((G - 1, PAD, LANES), F32),
            dma, dma, dma((2,)), dma((2,)), dma, dma,
            dma, dma, dma((2,)), dma((2,)), dma, dma,
            dma, dma, dma, dma, dma((sets,)), dma((sets,)), dma, dma,
        ],
        compiler_params=pltpu.CompilerParams(
            collective_id=0, has_side_effects=True, vmem_limit_bytes=56 * 2**20),
    )(source_pca, target_pca, source_labels.reshape(1, R), target_labels.reshape(1, C), block_mask)
    return pl.pallas_call(
        delivered,
        out_shape=tuple(jax.ShapeDtypeStruct(r.shape, F32) for r in raw),
        in_specs=[whole] * 2,
        out_specs=(pl.BlockSpec(memory_space=pl.ANY),) * 2,
        scratch_shapes=[dma((2,))],
    )(*(pltpu.with_memory_space_constraint(r, pltpu.VMEM) for r in raw))


def solution(mesh):
    placed = (P(None, "src"), P(None, "tgt"), P("src"), P("tgt"), P())
    return jax.shard_map(
        functools.partial(shards, mesh.shape["src"], mesh.shape["tgt"]),
        mesh=mesh,
        in_specs=placed,
        out_specs=(P(None, ("src", "tgt")), P(None, "tgt")),
        check_vma=False,
    )
```
